128 devices in a mesh: node: 64 (over z, y, x), hand: 2 (over core).
Axes of the slice: x: 4, y: 4, z: 4, core: 2. Of those that a mesh axis runs over, the one named last changes fastest.
Arguments:
- ranges: bfloat16 [2048, 128, 1326], P('node', None, 'hand'), may hold values from 0.00019931793 to 0.0039978027
- strengths: int32 [2048, 1326], P('node'), may hold values from 0 to 399
- live_hands: int32 [2048, 1326], P('node'), may hold values 0 or 1
- pot_sizes: float32 [2048, 128], P('node'), may hold values from 1 to 16
- action_counts: int32 [2048], P('node'), may hold values from 1 to 8
- parents: int32 [2048], P('node'), may hold values from 0 to 255
- turn_counts: int32 [64], replicated, may hold values from 1 to 4
- root_reach: float32 [64, 2, 1326], P(None, None, 'hand'), may hold values from 0.01 to 1
Outputs:
- turn_values: float32 [64, 2, 1326], P('node', None, 'hand')
- exploitability: float32 [], replicated
The draws below stay inside these ranges and needn't reach their ends.
All inputs are finite; a program needn't handle non-finite values. No bound on the sum of `live_hands` on one device may be relied on, other than what follows from the above.
Results may differ from the reference program's by a relative error of at most 0.0003.
Values may be sent and summed in bfloat16 or wider, within the bound.
A program may use at most 128 MiB of HBM per device.

```python
import math
import jax
import jax.numpy as jnp
import numpy as np
from jax import lax

H = 1326
ACT = 8
GROUPS = 8
TACT = 4
LINES = 64
NODES = 2048
TURNS = 64


def with_ends(values, rng, low, high):
    longest = values.shape.index(max(values.shape))
    spots = []
    for shift in (0, 1):
        where = [jax.random.randint(jax.random.fold_in(rng, axis), (), 0, length) for axis, length in enumerate(values.shape)]
        where[longest] = (where[longest] + shift) % values.shape[longest]
        spots.append(tuple(where))
    return values.at[spots[0]].set(low).at[spots[1]].set(high)


def block_scale(rng, extent, cuts, low, top_value):
    factor_of = 1.0
    for dim, blocks in cuts:
        steps = jax.random.uniform(jax.random.fold_in(jax.random.fold_in(rng, 6), dim), (blocks,), jnp.float32, low / len(cuts), top_value / len(cuts))
        factor_of = factor_of * jnp.repeat(jnp.exp(steps), extent[dim] // blocks).reshape((-1,) + (1,) * (len(extent) - 1 - dim))
    return factor_of


def setup_inputs(seed: int = 0) -> dict:
    key_of = jax.random.split(jax.random.key(seed), 9)
    ranges = jnp.clip(jnp.exp(math.log(0.0039978027) - 2.998599 * jax.random.uniform(key_of[0], (NODES, 2 * LINES, H), jnp.float32) ** block_scale(key_of[0], (NODES, 2 * LINES, H), ((0, 64), (2, 2)), -0.2, 0.2)), 0.00019931793, 0.0039978027).astype(jnp.bfloat16)
    strengths = with_ends(jax.random.randint(key_of[1], (NODES, H), 0, 400), jax.random.fold_in(key_of[1], 1), 0, 399).astype(jnp.int32)
    live_hands = with_ends((jax.random.randint(key_of[2], (NODES, H), 0, 10) < 9).astype(jnp.int32), jax.random.fold_in(key_of[2], 1), 0, 1)
    pot_sizes = jnp.clip(jnp.exp(math.log(16.0) - 2.7725887 * jax.random.uniform(key_of[3], (NODES, 2 * LINES), jnp.float32) ** block_scale(key_of[3], (NODES, 2 * LINES), ((0, 64),), -0.2, 0.2)), 1.0, 16.0)
    action_counts = with_ends(jax.random.randint(key_of[4], (NODES,), 1, ACT + 1), jax.random.fold_in(key_of[4], 1), 1, ACT).astype(jnp.int32)
    parents = with_ends(jax.random.randint(key_of[5], (NODES,), 0, TURNS * TACT), jax.random.fold_in(key_of[5], 1), 0, (TURNS * TACT) - 1).astype(jnp.int32)
    turn_counts = with_ends(jax.random.randint(key_of[6], (TURNS,), 1, TACT + 1), jax.random.fold_in(key_of[6], 1), 1, TACT).astype(jnp.int32)
    root_reach = jnp.clip(jnp.exp(math.log(1.0) - 4.6051702 * jax.random.uniform(key_of[7], (TURNS, 2, H), jnp.float32) ** block_scale(key_of[7], (TURNS, 2, H), ((2, 2),), -0.2, 0.2)), 0.01, 1.0)
    return dict(ranges=ranges, strengths=strengths, live_hands=live_hands, pot_sizes=pot_sizes, action_counts=action_counts, parents=parents, turn_counts=turn_counts, root_reach=root_reach)


def card_pairs(wanted):
    first_list = []
    second_list = []
    for lower_card in range(52):
        for upper_card in range(lower_card + 1, 52):
            first_list.append(lower_card)
            second_list.append(upper_card)
    return (jnp.asarray(np.array(first_list[:wanted], dtype=np.int32)),
            jnp.asarray(np.array(second_list[:wanted], dtype=np.int32)))


def pair_compat(row_first, row_second, col_first, col_second):
    shared = (row_first[:, None] == col_first[None, :]) | (row_first[:, None] == col_second[None, :])
    shared = shared | (row_second[:, None] == col_first[None, :]) | (row_second[:, None] == col_second[None, :])
    return jnp.where(shared, 0.0, 1.0).astype(jnp.float32)


def reference(ranges, strengths, live_hands, pot_sizes, action_counts, parents, turn_counts, root_reach):
    first_card, second_card = card_pairs(H)
    compat = pair_compat(first_card, second_card, first_card, second_card)

    def node_best(packed):
        strength, live_row, reach_rows, pot_row, legal = packed
        live_float = live_row.astype(jnp.float32)
        signs = jnp.sign((strength[:, None] - strength[None, :]).astype(jnp.float32))
        matrix = signs * compat * live_float[:, None] * live_float[None, :]
        values = jnp.dot(reach_rows.astype(jnp.float32), matrix.T, precision=lax.Precision.HIGHEST)
        values = (values * pot_row[:, None]).reshape(2, GROUPS, ACT, H)
        usable = jnp.arange(ACT) < legal
        best = jnp.where(usable[None, None, :, None], values, -1e30).max(axis=2)
        return jnp.sum(best, axis=1)

    river_best = lax.map(node_best, (strengths, live_hands, ranges, pot_sizes, action_counts))
    sums = jax.ops.segment_sum(river_best, parents, num_segments=TURNS * TACT)
    sums = sums.reshape(TURNS, TACT, 2, H)
    usable = jnp.arange(TACT)[None, :] < turn_counts[:, None]
    turn_values = jnp.where(usable[:, :, None, None], sums, -1e30).max(axis=1)
    exploitability = jnp.sum(root_reach * turn_values)
    return turn_values, exploitability
```

```python
import functools

import jax
import jax.numpy as jnp
import numpy as np
from jax import lax
from jax.experimental import pallas as pl
from jax.experimental.pallas import tpu as pltpu
from jax.sharding import Mesh
from jax.sharding import PartitionSpec as P

AXES = ("node_0", "node_1", "node_2", "hand")
NODE = AXES[:3]
MESH_ID = pl.DeviceIdType.MESH
F32 = jnp.float32
BF16 = jnp.bfloat16

ACT = 8
GROUPS = 8
TACT = 4
LINES = 128
HALF = 663
WIDE = 768
LOCAL = 32
MINE = 16
EARLY = 11
K_TILES = ((0, 256, 256), (256, 256, 256), (512, 160, 151))


def card_rows():
    first, second = np.triu_indices(52, 1)
    rows = np.zeros((8, WIDE), np.float32)
    for half in range(2):
        part = slice(half * HALF, (half + 1) * HALF)
        rows[half, :HALF] = first[part]
        rows[2 + half, :HALF] = second[part]
    return rows


def tall(row, rows):
    width = row.shape[1]
    block = jnp.broadcast_to(row, (16, width)).astype(BF16)
    return jnp.broadcast_to(block[None], (rows // 16, 16, width)).reshape(rows, width)


def turned(row):
    return jnp.broadcast_to(row, (128, 128)).T


def kernel(
    sizes,
    ranges,
    strengths,
    live,
    pots,
    counts,
    parents,
    turn_counts,
    reach,
    cards,
    turn_out,
    total_out,
    own_ranges,
    other_ranges,
    masked,
    s_rows,
    live_rows,
    pot_rows,
    s_columns,
    allow,
    forbid,
    partial,
    gathered,
    outgoing,
    keys,
    sums,
    arrived,
    my_reach,
    plane_part,
    plane_got,
    line_part,
    line_got,
    own_sem,
    other_sem,
    ranges_send,
    line_recv,
    line_send,
    key_recv,
    key_send,
    plane_recv,
    plane_send,
    reach_sem,
    b1_recv,
    b1_send,
    b2_recv,
    b2_send,
):
    place = [lax.axis_index(name) for name in NODE]
    core = lax.axis_index("hand")
    far = 1 - core
    turn = (place[0] * sizes[1] + place[1]) * sizes[2] + place[2]
    planes = ((1, 2), (0, 2), (0, 1))

    def at(where, which):
        return (where[0], where[1], where[2], which)

    def along(axis, step):
        where = list(place)
        where[axis] = lax.rem(place[axis] + step, sizes[axis])
        return where

    def plane_size(axis):
        high, low = planes[axis]
        return sizes[high] * sizes[low]

    def plane_mine(axis):
        high, low = planes[axis]
        return place[high] * sizes[low] + place[low]

    def in_plane(axis, slot):
        high, low = planes[axis]
        where = list(place)
        where[high] = slot // sizes[low]
        where[low] = lax.rem(slot, sizes[low])
        return where

    peers = [at(place, far)]
    for axis in range(3):
        for step in range(1, sizes[axis]):
            peers += [at(along(axis, step), which) for which in (core, far)]
    for axis in range(3):
        high, low = planes[axis]
        for up in range(1, sizes[high]):
            for side in range(1, sizes[low]):
                where = list(place)
                where[high] = lax.rem(place[high] + up, sizes[high])
                where[low] = lax.rem(place[low] + side, sizes[low])
                peers.append(at(where, core))

    barrier = pltpu.get_barrier_semaphore()
    for peer in peers:
        pl.semaphore_signal(barrier, inc=1, device_id=peer, device_id_type=MESH_ID)

    first = core * MINE
    for n in range(MINE):
        pltpu.make_async_copy(ranges.at[first + n], own_ranges.at[n], own_sem.at[n]).start()
    pltpu.make_async_copy(reach.at[turn], my_reach, reach_sem).start()

    rows = pl.ds(pl.multiple_of(first, MINE), MINE)
    s_rows[...] = jnp.zeros_like(s_rows)
    live_rows[...] = jnp.zeros_like(live_rows)
    for source, target, shift in ((strengths, s_rows, 200.0), (live, live_rows, 0.0)):
        low = source[rows, 0:HALF].astype(F32) - shift
        high = source[rows, HALF : 2 * HALF].astype(F32) - shift
        mine, theirs = jnp.where(core == 0, low, high), jnp.where(core == 0, high, low)
        for n in range(MINE):
            target[0, n, :, 0:HALF] = mine[n : n + 1]
            target[1, n, :, 0:HALF] = theirs[n : n + 1]
    my_pots = pots[rows, :]
    for n in range(MINE):
        pot_rows[n] = my_pots[n : n + 1]

    def pick(kind, half, lanes):
        low = cards[pl.ds(2 * kind, 1), lanes]
        high = cards[pl.ds(2 * kind + 1, 1), lanes]
        return jnp.where(core == half, low, high)

    lane = lax.broadcasted_iota(jnp.int32, (128, 128), 1)
    inside = (lane < HALF - 640).astype(F32).astype(BF16)

    def build(block, _):
        j_lanes = pl.ds(pl.multiple_of(block * 128, 128), 128)
        for j_half in range(2):
            a = turned(pick(0, j_half, j_lanes)).astype(BF16)
            b = turned(pick(1, j_half, j_lanes)).astype(BF16)
            for i_half in range(2):
                for i_block in range(6):
                    lanes = pl.ds(i_block * 128, 128)
                    c = tall(pick(0, i_half, lanes), 128)
                    d = tall(pick(1, i_half, lanes), 128)
                    apart = ((a - c) * (a - d)) * ((b - c) * (b - d))
                    one = jnp.minimum(jnp.abs(apart), jnp.ones_like(apart))
                    if i_block == 5:
                        one = one * inside
                    where = pl.ds(i_half * WIDE + i_block * 128, 128)
                    allow[j_half, j_lanes, where] = one
                    forbid[j_half, j_lanes, where] = -one
        return 0

    lax.fori_loop(0, 6, build, 0)

    def prepare(half, source, n):
        for block in range(6):
            lanes = pl.ds(block * 128, 128)
            s_columns[lanes, :] = turned(s_rows[half, n, :, lanes]).astype(BF16)
        for start, _, width in K_TILES:
            lanes = pl.ds(start, width)
            flags = tall(live_rows[half, n, :, lanes], LINES)
            masked[:, lanes] = source[n, :, lanes] * flags

    def product(half, n, tile):
        lanes = pl.ds((tile % 3) * 256, 256)
        s_lane = s_rows[tile // 3, n, :, lanes]
        added = None
        for start, tall_rows, width in K_TILES:
            inner = pl.ds(start, tall_rows)
            column = s_columns[inner, :]
            gap = tall(s_lane, tall_rows) - jnp.concatenate([column, column], axis=1)
            where = pl.ds(tile * 256, 256)
            sign = jnp.minimum(
                jnp.maximum(gap, forbid[half, inner, where]), allow[half, inner, where]
            )
            term = jnp.dot(
                masked[:, pl.ds(start, width)], sign[:width], preferred_element_type=F32
            )
            added = term if added is None else added + term
        return added

    def own_half(n, _):
        pltpu.make_async_copy(ranges.at[first + n], own_ranges.at[n], own_sem.at[n]).wait()
        prepare(0, own_ranges, n)
        for tile in range(6):
            partial[n, :, pl.ds(tile * 256, 256)] = product(0, n, tile)
        return 0

    def exchange(n):
        return pltpu.make_async_remote_copy(
            src_ref=ranges.at[far * MINE + n],
            dst_ref=other_ranges.at[n],
            send_sem=ranges_send.at[n],
            recv_sem=other_sem.at[n],
            device_id=at(place, far),
            device_id_type=MESH_ID,
        )

    lax.fori_loop(0, EARLY, own_half, 0)
    pl.semaphore_wait(barrier, len(peers))
    for n in range(MINE):
        exchange(n).start()

    lane_row = lax.broadcasted_iota(jnp.int32, (1, 128), 1)
    spread = jnp.zeros((1, 128), jnp.int32)
    for n in range(LOCAL):
        spread = jnp.where(lane_row // 4 == n, parents[n], spread)
    key_row = (spread * 4 + lax.rem(lane_row, 4)).astype(F32)

    def key_copy(axis, step):
        return pltpu.make_async_remote_copy(
            src_ref=keys.at[axis, 0],
            dst_ref=keys.at[axis, sizes[axis] - step],
            send_sem=key_send.at[axis, step],
            recv_sem=key_recv.at[axis, sizes[axis] - step],
            device_id=at(along(axis, step), core),
            device_id_type=MESH_ID,
        )

    for axis in range(3):
        keys[axis, 0] = key_row
        for step in range(1, sizes[axis]):
            key_copy(axis, step).start()

    lax.fori_loop(EARLY, MINE, own_half, 0)

    my_block = core * (MINE * 4)

    def river_copies(batch):
        copies = []
        from_rows = pl.ds(pl.multiple_of(batch * 8, 8), 8)
        mine = pl.ds(pl.multiple_of(my_block + batch * 8, 8), 8)
        for axis in range(3):
            send, recv = line_send.at[axis], line_recv.at[axis]
            for step in range(1, sizes[axis]):
                base = (sizes[axis] - step) * 128
                there = pl.ds(pl.multiple_of(base + my_block + batch * 8, 8), 8)
                for source, which in (
                    (gathered.at[axis, mine], core),
                    (outgoing.at[axis, from_rows], far),
                ):
                    copies.append(
                        pltpu.make_async_remote_copy(
                            src_ref=source,
                            dst_ref=gathered.at[axis, there],
                            send_sem=send,
                            recv_sem=recv,
                            device_id=at(along(axis, step), which),
                            device_id_type=MESH_ID,
                        )
                    )
            copies.append(
                pltpu.make_async_remote_copy(
                    src_ref=outgoing.at[axis, from_rows],
                    dst_ref=gathered.at[axis, mine],
                    send_sem=send,
                    recv_sem=recv,
                    device_id=at(place, far),
                    device_id_type=MESH_ID,
                )
            )
        return copies

    action = lax.rem(lax.broadcasted_iota(jnp.int32, (LINES, 256), 0), ACT)

    def other_half(n):
        exchange(n).wait_recv()
        prepare(1, other_ranges, n)
        usable = action < counts[first + n]
        pot = turned(pot_rows[n])
        pot = jnp.concatenate([pot, pot], axis=1)
        rivers = []
        for tile in range(6):
            values = product(1, n, tile) + partial[n, :, pl.ds(tile * 256, 256)]
            values = jnp.where(usable, values * pot, -1e30)
            best = values.reshape(2, GROUPS, ACT, 256).max(axis=2).sum(axis=1)
            best = best * live_rows[tile // 3, n, :, pl.ds((tile % 3) * 256, 256)]
            rivers.append(best)
        return rivers

    def two_nodes(batch, _):
        even, odd = other_half(2 * batch), other_half(2 * batch + 1)
        for tile in range(6):
            pieces = []
            for best in (even[tile], odd[tile]):
                for player in range(2):
                    for side in range(2):
                        lanes = slice(side * 128, side * 128 + 128)
                        pieces.append(best[player : player + 1, lanes])
            block = jnp.concatenate(pieces, axis=0)
            if tile < 3:
                gathered[tile, pl.ds(pl.multiple_of(my_block + batch * 8, 8), 8), :] = block
            else:
                outgoing[tile - 3, pl.ds(pl.multiple_of(batch * 8, 8), 8), :] = block
        for copy in river_copies(batch):
            copy.start()
        return 0

    lax.fori_loop(0, MINE // 2, two_nodes, 0)

    for axis in range(3):
        for step in range(1, sizes[axis]):
            key_copy(axis, step).wait_recv()

    for axis in range(3):
        count = plane_size(axis)
        q = lax.broadcasted_iota(jnp.int32, (count * 16, 128), 0)
        there = in_plane(axis, q // 16)
        owner = (there[0] * sizes[1] + there[1]) * sizes[2] + there[2]
        wanted = (owner * (TACT * 4) + lax.rem(q, 16)).astype(F32)
        lines = sizes[axis] * 128
        hot = jnp.concatenate(
            [
                jnp.where(wanted == keys[axis, e], 1.0, 0.0).astype(BF16)
                for e in range(sizes[axis])
            ],
            axis=1,
        )
        blocks = (sizes[axis] - 1) * 128 + 64
        whole = gathered.at[axis, pl.ds(0, blocks)]
        pltpu.make_async_copy(whole, whole, line_recv.at[axis]).wait()
        rows_in = gathered[axis, pl.ds(0, lines), :]
        upper = rows_in.astype(BF16)
        lower = (rows_in - upper.astype(F32)).astype(BF16)
        both = jnp.dot(hot, upper, preferred_element_type=F32) + jnp.dot(
            hot, lower, preferred_element_type=F32
        )
        sums[axis, pl.ds(0, count * 16), :] = both
        mine = plane_mine(axis)
        here = pl.ds(pl.multiple_of(mine * 16, 16), 16)
        for step in range(1, count):
            slot = lax.rem(mine + step, count)
            part = pl.ds(pl.multiple_of(slot * 16, 16), 16)
            pltpu.make_async_remote_copy(
                src_ref=sums.at[axis, part],
                dst_ref=arrived.at[axis, here],
                send_sem=plane_send.at[axis],
                recv_sem=plane_recv.at[axis],
                device_id=at(in_plane(axis, slot), core),
                device_id_type=MESH_ID,
            ).start()
        arrived[axis, here, :] = sums[axis, here, :]

    pltpu.make_async_copy(reach.at[turn], my_reach, reach_sem).wait()
    legal = turn_counts[turn]
    spot = lax.broadcasted_iota(jnp.int32, (1, 128), 1)
    weighed = jnp.zeros((1, 128), F32)
    for axis in range(3):
        count = plane_size(axis)
        whole = arrived.at[axis, pl.ds(0, (count - 1) * 16)]
        pltpu.make_async_copy(whole, whole, plane_recv.at[axis]).wait()
        total = arrived[axis, pl.ds(0, count * 16), :].reshape(count, 16, 128).sum(axis=0)
        best = total[0:4]
        for a in range(1, TACT):
            best = jnp.maximum(best, jnp.where(a < legal, total[4 * a : 4 * a + 4], -1e30))
        for player in range(2):
            for side in range(2):
                piece = best[player * 2 + side : player * 2 + side + 1]
                start = axis * 256 + side * 128
                width = min(128, HALF - start)
                lanes = pl.ds(start, width)
                turn_out[0, pl.ds(player, 1), lanes] = piece[:, :width]
                part = piece[:, :width] * my_reach[pl.ds(player, 1), lanes]
                if width == 128:
                    weighed = weighed + part
                else:
                    weighed = weighed + jnp.where(
                        spot == 0, jnp.sum(part, axis=1, keepdims=True), 0.0
                    )

    count = plane_size(2)
    mine = plane_mine(2)
    plane_part[0] = weighed
    plane_got[mine] = weighed

    def first_hop(step):
        slot = lax.rem(mine + step, count)
        return pltpu.make_async_remote_copy(
            src_ref=plane_part.at[0],
            dst_ref=plane_got.at[mine],
            send_sem=b1_send,
            recv_sem=b1_recv,
            device_id=at(in_plane(2, slot), core),
            device_id_type=MESH_ID,
        )

    for step in range(1, count):
        first_hop(step).start()
    whole = plane_got.at[pl.ds(0, count - 1)]
    pltpu.make_async_copy(whole, whole, b1_recv).wait()
    weighed = plane_got[...].sum(axis=0)
    slots = sizes[2] * 2
    slot = place[2] * 2 + core
    line_part[0] = weighed
    line_got[slot] = weighed

    def second_hop(step, which):
        return pltpu.make_async_remote_copy(
            src_ref=line_part.at[0],
            dst_ref=line_got.at[slot],
            send_sem=b2_send,
            recv_sem=b2_recv,
            device_id=at(along(2, step), which),
            device_id_type=MESH_ID,
        )

    second_hop(0, far).start()
    for step in range(1, sizes[2]):
        second_hop(step, core).start()
        second_hop(step, far).start()

    for n in range(MINE):
        exchange(n).wait_send()
    for axis in range(3):
        for step in range(1, sizes[axis]):
            key_copy(axis, step).wait_send()
        sent = gathered.at[axis, pl.ds(0, (sizes[axis] - 1) * 64)]
        for _ in range(2):
            pltpu.make_async_copy(sent, sent, line_send.at[axis]).wait()
        sent = gathered.at[axis, pl.ds(0, 64)]
        pltpu.make_async_copy(sent, sent, line_send.at[axis]).wait()
        sent = arrived.at[axis, pl.ds(0, (plane_size(axis) - 1) * 16)]
        pltpu.make_async_copy(sent, sent, plane_send.at[axis]).wait()
    sent = plane_got.at[pl.ds(0, count - 1)]
    pltpu.make_async_copy(sent, sent, b1_send).wait()
    sent = line_got.at[pl.ds(0, slots - 1)]
    pltpu.make_async_copy(sent, sent, b2_send).wait()
    pltpu.make_async_copy(sent, sent, b2_recv).wait()
    total_out[0, 0] = jnp.sum(line_got[...].sum(axis=0))


def local(sizes, ranges, strengths, live, pots, counts, parents, turn_counts, reach):
    dma = pltpu.SemaphoreType.DMA
    longest = max(sizes)
    widest = max(sizes[0] * sizes[1], sizes[1] * sizes[2], sizes[0] * sizes[2])
    vmem = pl.BlockSpec(memory_space=pltpu.VMEM)
    smem = pl.BlockSpec(memory_space=pltpu.SMEM)
    hbm = pl.BlockSpec(memory_space=pl.ANY)
    turn_values, total = pl.pallas_call(
        functools.partial(kernel, sizes),
        out_shape=(
            jax.ShapeDtypeStruct((1, 2, HALF), F32),
            jax.ShapeDtypeStruct((1, 1), F32),
        ),
        in_specs=[hbm, vmem, vmem, vmem, smem, smem, smem, hbm, vmem],
        out_specs=(vmem, smem),
        scratch_shapes=[
            pltpu.VMEM((MINE, LINES, HALF), BF16),
            pltpu.VMEM((MINE, LINES, HALF), BF16),
            pltpu.VMEM((LINES, HALF), BF16),
            pltpu.VMEM((2, MINE, 1, WIDE), F32),
            pltpu.VMEM((2, MINE, 1, WIDE), F32),
            pltpu.VMEM((MINE, 1, LINES), F32),
            pltpu.VMEM((WIDE, 128), BF16),
            pltpu.VMEM((2, WIDE, 2 * WIDE), BF16),
            pltpu.VMEM((2, WIDE, 2 * WIDE), BF16),
            pltpu.VMEM((MINE, LINES, 2 * WIDE), F32),
            pltpu.VMEM((3, longest * 128, 128), F32),
            pltpu.VMEM((3, 64, 128), F32),
            pltpu.VMEM((3, longest, 1, 128), F32),
            pltpu.VMEM((3, widest * 16, 128), F32),
            pltpu.VMEM((3, widest * 16, 128), F32),
            pltpu.VMEM((2, HALF), F32),
            pltpu.VMEM((1, 1, 128), F32),
            pltpu.VMEM((sizes[0] * sizes[1], 1, 128), F32),
            pltpu.VMEM((1, 1, 128), F32),
            pltpu.VMEM((sizes[2] * 2, 1, 128), F32),
            dma((MINE,)),
            dma((MINE,)),
            dma((MINE,)),
            dma((3,)),
            dma((3,)),
            dma((3, longest)),
            dma((3, longest)),
            dma((3,)),
            dma((3,)),
            dma(()),
            dma(()),
            dma(()),
            dma(()),
            dma(()),
        ],
        compiler_params=pltpu.CompilerParams(
            collective_id=0, has_side_effects=True, vmem_limit_bytes=60 * 1024 * 1024
        ),
    )(
        ranges,
        strengths,
        live,
        pots,
        counts,
        parents,
        turn_counts,
        reach,
        jnp.asarray(card_rows()),
    )
    return turn_values, total[0, 0]


def solution(mesh):
    sides = {128: (4, 4, 4), 16: (2, 2, 2)}[mesh.devices.size]
    split = Mesh(mesh.devices.reshape(*sides, 2), AXES)
    in_specs = (
        P(NODE, None, "hand"),
        P(NODE, None),
        P(NODE, None),
        P(NODE, None),
        P(NODE),
        P(NODE),
        P(),
        P(None, None, "hand"),
    )
    out_specs = (P(NODE, None, "hand"), P())
    return jax.shard_map(
        functools.partial(local, sides),
        mesh=split,
        in_specs=in_specs,
        out_specs=out_specs,
        check_vma=False,
    )
```

```python
import functools

import jax
import jax.numpy as jnp
import numpy as np
from jax import lax
from jax.experimental import pallas as pl
from jax.experimental.pallas import tpu as pltpu
from jax.sharding import Mesh
from jax.sharding import PartitionSpec as P

AXES = ("node_0", "node_1", "node_2", "hand")
NODE = AXES[:3]
MESH_ID = pl.DeviceIdType.MESH
F32 = jnp.float32
BF16 = jnp.bfloat16

ACT = 8
GROUPS = 8
TACT = 4
LINES = 128
HALF = 663
WIDE = 768
LOCAL = 32
MINE = 16
EARLY = 5
TALL = 672
K_TILES = ((0, 256), (256, 256), (512, 160))
J_BLOCKS = tuple((b * 128, min(128, HALF - b * 128)) for b in range(6))


def card_hots():
    first, second = np.triu_indices(52, 1)
    hots = np.zeros((4, WIDE, 64), np.float32)
    for half in range(2):
        for h in range(HALF):
            cards = [first[half * HALF + h], second[half * HALF + h]]
            hots[half, h, cards] = 1.0
            hots[2 + half, h, cards] = -1.0
            hots[2 + half, h, 52] = 1.0
        hots[half, :, 52] = 1.0
    return hots


def tall(row, rows):
    width = row.shape[1]
    block = jnp.broadcast_to(row, (16, width)).astype(BF16)
    return jnp.broadcast_to(block[None], (rows // 16, 16, width)).reshape(rows, width)


def turned(row):
    return jnp.broadcast_to(row, (128, 128)).T


def merged(parts, reduce):
    row = lax.broadcasted_iota(jnp.int32, (8, 128), 0)
    for bit in (1, 2, 4):
        low = (row & bit) == 0
        pairs = []
        for one, two in zip(parts[::2], parts[1::2]):
            kept = jnp.where(low, one, two)
            moved = pltpu.roll(jnp.where(low, two, one), 8 - bit, axis=0)
            pairs.append(reduce(kept, moved))
        parts = pairs
    return parts[0]


def kernel(
    sizes,
    ranges,
    strengths,
    live,
    pots,
    counts,
    parents,
    turn_counts,
    reach,
    hots,
    turn_out,
    total_out,
    raw,
    by_node,
    masked,
    s_rows,
    live_rows,
    pot_rows,
    s_columns,
    allow,
    forbid,
    pot_columns,
    partial,
    hot,
    gathered,
    outgoing,
    keys,
    sums,
    arrived,
    my_reach,
    plane_part,
    plane_got,
    line_part,
    line_got,
    own_sem,
    other_sem,
    ranges_send,
    line_recv,
    line_send,
    key_recv,
    key_send,
    plane_recv,
    plane_send,
    reach_sem,
    b1_recv,
    b1_send,
    b2_recv,
    b2_send,
):
    place = [lax.axis_index(name) for name in NODE]
    core = lax.axis_index("hand")
    far = 1 - core
    turn = (place[0] * sizes[1] + place[1]) * sizes[2] + place[2]
    planes = ((1, 2), (0, 2), (0, 1))

    def at(where, which):
        return (where[0], where[1], where[2], which)

    def along(axis, step):
        where = list(place)
        where[axis] = lax.rem(place[axis] + step, sizes[axis])
        return where

    def plane_size(axis):
        high, low = planes[axis]
        return sizes[high] * sizes[low]

    def plane_mine(axis):
        high, low = planes[axis]
        return place[high] * sizes[low] + place[low]

    def in_plane(axis, slot):
        high, low = planes[axis]
        where = list(place)
        where[high] = slot // sizes[low]
        where[low] = lax.rem(slot, sizes[low])
        return where

    peers = [at(place, far)]
    for axis in range(3):
        for step in range(1, sizes[axis]):
            peers += [at(along(axis, step), which) for which in (core, far)]
    for axis in range(3):
        high, low = planes[axis]
        for up in range(1, sizes[high]):
            for side in range(1, sizes[low]):
                where = list(place)
                where[high] = lax.rem(place[high] + up, sizes[high])
                where[low] = lax.rem(place[low] + side, sizes[low])
                peers.append(at(where, core))

    barrier = pltpu.get_barrier_semaphore()
    for peer in peers:
        pl.semaphore_signal(barrier, inc=1, device_id=peer, device_id_type=MESH_ID)

    first = core * MINE
    def fetch(block):
        start, width = J_BLOCKS[block]
        return pltpu.make_async_copy(
            ranges.at[pl.ds(start, width), pl.ds(pl.multiple_of(first, MINE), MINE)],
            raw.at[0, pl.ds(start, width)],
            own_sem.at[block],
        )

    def exchange(block):
        start, width = J_BLOCKS[block]
        theirs = pl.ds(pl.multiple_of(far * MINE, MINE), MINE)
        return pltpu.make_async_remote_copy(
            src_ref=ranges.at[pl.ds(start, width), theirs],
            dst_ref=raw.at[1, pl.ds(start, width)],
            send_sem=ranges_send.at[block],
            recv_sem=other_sem.at[block],
            device_id=at(place, far),
            device_id_type=MESH_ID,
        )

    for block in range(6):
        fetch(block).start()
    pltpu.make_async_copy(reach.at[turn], my_reach, reach_sem).start()

    rows = pl.ds(pl.multiple_of(first, MINE), MINE)
    s_rows[...] = jnp.full_like(s_rows, -1000.0)
    live_rows[...] = jnp.zeros_like(live_rows)
    for source, target, shift in ((strengths, s_rows, 200.0), (live, live_rows, 0.0)):
        low = source[rows, 0:HALF].astype(F32) - shift
        high = source[rows, HALF : 2 * HALF].astype(F32) - shift
        mine, theirs = jnp.where(core == 0, low, high), jnp.where(core == 0, high, low)
        for n in range(MINE):
            target[0, n, :, 0:HALF] = mine[n : n + 1]
            target[1, n, :, 0:HALF] = theirs[n : n + 1]
    my_pots = pots[rows, :]
    for n in range(MINE):
        pot_rows[n] = my_pots[n : n + 1]

    def build(group, _):
        lanes = pl.ds(pl.multiple_of(group * 256, 256), 256)
        for j_half, j_core in enumerate((core, far)):
            for i_half, i_core in enumerate((core, far)):
                free = lax.dot_general(
                    hots[j_core, 0:TALL, :],
                    hots[2 + i_core, lanes, :],
                    (((1,), (1,)), ((), ())),
                    preferred_element_type=F32,
                ).astype(BF16)
                for side in range(2):
                    part = free[:, side * 128 : side * 128 + 128]
                    zero = jnp.zeros_like(part)
                    where = i_half * 6 + group * 2 + side
                    allow[j_half, where] = jnp.maximum(part, zero)
                    forbid[j_half, where] = jnp.minimum(-part, zero)
        return 0

    lax.fori_loop(0, 3, build, 0)

    def swap(half, wait):
        for block in range(6):
            wait(block)

        def one(block, _):
            rows = pl.ds(pl.multiple_of(block * 128, 128), 128)
            by_node[half, :, rows, :] = jnp.swapaxes(raw[half, rows], 0, 1)
            return 0

        lax.fori_loop(0, 5, one, 0)
        by_node[half, :, 640:TALL, :] = jnp.swapaxes(raw[half, 640:TALL], 0, 1)

    lane = lax.broadcasted_iota(jnp.int32, (LINES, 128), 1)
    action = lax.rem(lax.broadcasted_iota(jnp.int32, (LINES, 128), 0), ACT)

    def prepare(half, n, slot):
        for block in range(6):
            lanes = pl.ds(block * 128, 128)
            flags = tall(live_rows[half, n, :, lanes], LINES)
            if block < 5:
                s_columns[slot, lanes, :] = turned(s_rows[half, n, :, lanes].astype(BF16))
                masked[slot, block] = by_node[half, n, lanes, :].T * flags
            else:
                column = turned(s_rows[half, n, :, lanes].astype(BF16))
                s_columns[slot, 640:TALL, :] = column[: TALL - 640]
                last = by_node[half, n, 640:TALL, :]
                last = jnp.concatenate([last, jnp.zeros((96, 128), BF16)], axis=0).T
                last = (last * flags).astype(F32)
                bar = jnp.where(action < counts[first + n], 0.0, -1024.0)
                bar = jnp.where(lane == HALF - 640, bar, 0.0)
                masked[slot, block] = jnp.where(lane < HALF - 640, last, bar).astype(BF16)

    def product(half, n, slot, tile):
        added = None
        for step, (start, height) in enumerate(K_TILES):
            inner = pl.ds(start, height)
            column = s_columns[slot, inner, :]
            signs = []
            for side in range(2):
                lanes = pl.ds((tile % 3) * 256 + side * 128, 128)
                gap = tall(s_rows[tile // 3, n, :, lanes], height) - column
                where = tile * 2 + side
                signs.append(
                    jnp.minimum(
                        jnp.maximum(gap, forbid[half, where, inner, :]),
                        allow[half, where, inner, :],
                    )
                )
            left = jnp.concatenate([masked[slot, 2 * step], masked[slot, 2 * step + 1]], axis=1)
            term = jnp.dot(
                left[:, :height],
                jnp.concatenate(signs, axis=1),
                preferred_element_type=F32,
            )
            added = term if added is None else added + term
        return added

    def own_half(pair, _):
        for slot in range(2):
            prepare(0, 2 * pair + slot, slot)
        for slot in range(2):
            n = 2 * pair + slot
            for tile in range(6):
                partial[n, :, pl.ds(tile * 256, 256)] = product(0, n, slot, tile)
        return 0

    swap(0, lambda block: fetch(block).wait())
    lax.fori_loop(0, EARLY, own_half, 0)
    pl.semaphore_wait(barrier, len(peers))
    for block in range(6):
        exchange(block).start()

    lane_row = lax.broadcasted_iota(jnp.int32, (1, 128), 1)
    spread = jnp.zeros((1, 128), jnp.int32)
    for n in range(LOCAL):
        spread = jnp.where(lane_row // 4 == n, parents[n], spread)
    key_row = (spread * 4 + lax.rem(lane_row, 4)).astype(F32)

    def key_copy(axis, step):
        return pltpu.make_async_remote_copy(
            src_ref=keys.at[axis, 0],
            dst_ref=keys.at[axis, sizes[axis] - step],
            send_sem=key_send.at[axis, step],
            recv_sem=key_recv.at[axis, sizes[axis] - step],
            device_id=at(along(axis, step), core),
            device_id_type=MESH_ID,
        )

    for axis in range(3):
        keys[axis, 0] = key_row
        for step in range(1, sizes[axis]):
            key_copy(axis, step).start()

    lax.fori_loop(EARLY, MINE // 2, own_half, 0)
    swap(1, lambda block: exchange(block).wait_recv())

    my_block = core * (MINE * 4)

    def river_copies(batch):
        copies = []
        from_rows = pl.ds(pl.multiple_of(batch * 8, 8), 8)
        mine = pl.ds(pl.multiple_of(my_block + batch * 8, 8), 8)
        for axis in range(3):
            send, recv = line_send.at[axis], line_recv.at[axis]
            for step in range(1, sizes[axis]):
                base = (sizes[axis] - step) * 128
                there = pl.ds(pl.multiple_of(base + my_block + batch * 8, 8), 8)
                for source, which in (
                    (gathered.at[axis, mine], core),
                    (outgoing.at[axis, from_rows], far),
                ):
                    copies.append(
                        pltpu.make_async_remote_copy(
                            src_ref=source,
                            dst_ref=gathered.at[axis, there],
                            send_sem=send,
                            recv_sem=recv,
                            device_id=at(along(axis, step), which),
                            device_id_type=MESH_ID,
                        )
                    )
            copies.append(
                pltpu.make_async_remote_copy(
                    src_ref=outgoing.at[axis, from_rows],
                    dst_ref=gathered.at[axis, mine],
                    send_sem=send,
                    recv_sem=recv,
                    device_id=at(place, far),
                    device_id_type=MESH_ID,
                )
            )
        return copies

    def two_nodes(batch, _):
        for slot in range(2):
            n = 2 * batch + slot
            prepare(1, n, slot)
            pot_columns[slot] = turned(pot_rows[n])
        for tile in range(6):
            rows = []
            for slot in range(2):
                n = 2 * batch + slot
                values = product(1, n, slot, tile) + partial[n, :, pl.ds(tile * 256, 256)]
                for player in range(2):
                    for side in range(2):
                        start = (tile % 3) * 256 + side * 128
                        parts = []
                        for g in range(GROUPS):
                            at_row = (player * GROUPS + g) * ACT
                            part = values[at_row : at_row + 8, side * 128 : side * 128 + 128]
                            parts.append(part * pot_columns[slot, at_row : at_row + 8, :])
                        best = merged(parts, jnp.maximum)
                        rows.append(best * live_rows[tile // 3, n, :, pl.ds(start, 128)])
            block = merged(rows, jnp.add)
            if tile < 3:
                gathered[tile, pl.ds(pl.multiple_of(my_block + batch * 8, 8), 8), :] = block
            else:
                outgoing[tile - 3, pl.ds(pl.multiple_of(batch * 8, 8), 8), :] = block
        for copy in river_copies(batch):
            copy.start()
        return 0

    lax.fori_loop(0, MINE // 2, two_nodes, 0)

    for axis in range(3):
        for step in range(1, sizes[axis]):
            key_copy(axis, step).wait_recv()

    for axis in range(3):
        count = plane_size(axis)
        q = lax.broadcasted_iota(jnp.int32, (count * 16, 128), 0)
        there = in_plane(axis, q // 16)
        owner = (there[0] * sizes[1] + there[1]) * sizes[2] + there[2]
        wanted = (owner * (TACT * 4) + lax.rem(q, 16)).astype(F32)
        for e in range(sizes[axis]):
            hit = jnp.where(wanted == keys[axis, e], 1.0, 0.0).astype(BF16)
            hot[axis, e, 0 : count * 16, :] = hit

    for axis in range(3):
        count = plane_size(axis)
        lines = sizes[axis] * 128
        blocks = (sizes[axis] - 1) * 128 + 64
        whole = gathered.at[axis, pl.ds(0, blocks)]
        pltpu.make_async_copy(whole, whole, line_recv.at[axis]).wait()
        rows_in = gathered[axis, pl.ds(0, lines), :]
        upper = rows_in.astype(BF16)
        lower = (rows_in - upper.astype(F32)).astype(BF16)
        left = jnp.concatenate(
            [hot[axis, e, 0 : count * 16, :] for e in range(sizes[axis])], axis=1
        )
        both = jnp.dot(left, upper, preferred_element_type=F32) + jnp.dot(
            left, lower, preferred_element_type=F32
        )
        sums[axis, pl.ds(0, count * 16), :] = both
        mine = plane_mine(axis)
        here = pl.ds(pl.multiple_of(mine * 16, 16), 16)
        for step in range(1, count):
            slot = lax.rem(mine + step, count)
            part = pl.ds(pl.multiple_of(slot * 16, 16), 16)
            pltpu.make_async_remote_copy(
                src_ref=sums.at[axis, part],
                dst_ref=arrived.at[axis, here],
                send_sem=plane_send.at[axis],
                recv_sem=plane_recv.at[axis],
                device_id=at(in_plane(axis, slot), core),
                device_id_type=MESH_ID,
            ).start()
        arrived[axis, here, :] = sums[axis, here, :]

    pltpu.make_async_copy(reach.at[turn], my_reach, reach_sem).wait()
    legal = turn_counts[turn]
    spot = lax.broadcasted_iota(jnp.int32, (1, 128), 1)
    weighed = jnp.zeros((1, 128), F32)
    for axis in range(3):
        count = plane_size(axis)
        whole = arrived.at[axis, pl.ds(0, (count - 1) * 16)]
        pltpu.make_async_copy(whole, whole, plane_recv.at[axis]).wait()
        total = arrived[axis, pl.ds(0, count * 16), :].reshape(count, 16, 128).sum(axis=0)
        best = total[0:4]
        for a in range(1, TACT):
            best = jnp.maximum(best, jnp.where(a < legal, total[4 * a : 4 * a + 4], -1e30))
        for player in range(2):
            for side in range(2):
                piece = best[player * 2 + side : player * 2 + side + 1]
                start = axis * 256 + side * 128
                width = min(128, HALF - start)
                lanes = pl.ds(start, width)
                turn_out[0, pl.ds(player, 1), lanes] = piece[:, :width]
                part = piece[:, :width] * my_reach[pl.ds(player, 1), lanes]
                if width == 128:
                    weighed = weighed + part
                else:
                    weighed = weighed + jnp.where(
                        spot == 0, jnp.sum(part, axis=1, keepdims=True), 0.0
                    )

    count = plane_size(2)
    mine = plane_mine(2)
    plane_part[0] = weighed
    plane_got[mine] = weighed

    def first_hop(step):
        slot = lax.rem(mine + step, count)
        return pltpu.make_async_remote_copy(
            src_ref=plane_part.at[0],
            dst_ref=plane_got.at[mine],
            send_sem=b1_send,
            recv_sem=b1_recv,
            device_id=at(in_plane(2, slot), core),
            device_id_type=MESH_ID,
        )

    for step in range(1, count):
        first_hop(step).start()
    whole = plane_got.at[pl.ds(0, count - 1)]
    pltpu.make_async_copy(whole, whole, b1_recv).wait()
    weighed = plane_got[...].sum(axis=0)
    slots = sizes[2] * 2
    slot = place[2] * 2 + core
    line_part[0] = weighed
    line_got[slot] = weighed

    def second_hop(step, which):
        return pltpu.make_async_remote_copy(
            src_ref=line_part.at[0],
            dst_ref=line_got.at[slot],
            send_sem=b2_send,
            recv_sem=b2_recv,
            device_id=at(along(2, step), which),
            device_id_type=MESH_ID,
        )

    second_hop(0, far).start()
    for step in range(1, sizes[2]):
        second_hop(step, core).start()
        second_hop(step, far).start()

    for block in range(6):
        exchange(block).wait_send()
    for axis in range(3):
        for step in range(1, sizes[axis]):
            key_copy(axis, step).wait_send()
        sent = gathered.at[axis, pl.ds(0, (sizes[axis] - 1) * 64)]
        for _ in range(2):
            pltpu.make_async_copy(sent, sent, line_send.at[axis]).wait()
        sent = gathered.at[axis, pl.ds(0, 64)]
        pltpu.make_async_copy(sent, sent, line_send.at[axis]).wait()
        sent = arrived.at[axis, pl.ds(0, (plane_size(axis) - 1) * 16)]
        pltpu.make_async_copy(sent, sent, plane_send.at[axis]).wait()
    sent = plane_got.at[pl.ds(0, count - 1)]
    pltpu.make_async_copy(sent, sent, b1_send).wait()
    sent = line_got.at[pl.ds(0, slots - 1)]
    pltpu.make_async_copy(sent, sent, b2_send).wait()
    pltpu.make_async_copy(sent, sent, b2_recv).wait()
    total_out[0, 0] = jnp.sum(line_got[...].sum(axis=0))


def local(sizes, ranges, strengths, live, pots, counts, parents, turn_counts, reach):
    dma = pltpu.SemaphoreType.DMA
    longest = max(sizes)
    widest = max(sizes[0] * sizes[1], sizes[1] * sizes[2], sizes[0] * sizes[2])
    vmem = pl.BlockSpec(memory_space=pltpu.VMEM)
    smem = pl.BlockSpec(memory_space=pltpu.SMEM)
    hbm = pl.BlockSpec(memory_space=pl.ANY)
    turn_values, total = pl.pallas_call(
        functools.partial(kernel, sizes),
        out_shape=(
            jax.ShapeDtypeStruct((1, 2, HALF), F32),
            jax.ShapeDtypeStruct((1, 1), F32),
        ),
        in_specs=[hbm, vmem, vmem, vmem, smem, smem, smem, hbm, vmem],
        out_specs=(vmem, smem),
        scratch_shapes=[
            pltpu.VMEM((2, TALL, MINE, LINES), BF16),
            pltpu.VMEM((2, MINE, TALL, LINES), BF16),
            pltpu.VMEM((2, 6, LINES, 128), BF16),
            pltpu.VMEM((2, MINE, 1, WIDE), F32),
            pltpu.VMEM((2, MINE, 1, WIDE), F32),
            pltpu.VMEM((MINE, 1, LINES), F32),
            pltpu.VMEM((2, TALL, 128), BF16),
            pltpu.VMEM((2, 12, TALL, 128), BF16),
            pltpu.VMEM((2, 12, TALL, 128), BF16),
            pltpu.VMEM((2, LINES, 128), F32),
            pltpu.VMEM((MINE, LINES, 2 * WIDE), F32),
            pltpu.VMEM((3, longest, widest * 16, 128), BF16),
            pltpu.VMEM((3, longest * 128, 128), F32),
            pltpu.VMEM((3, 64, 128), F32),
            pltpu.VMEM((3, longest, 1, 128), F32),
            pltpu.VMEM((3, widest * 16, 128), F32),
            pltpu.VMEM((3, widest * 16, 128), F32),
            pltpu.VMEM((2, HALF), F32),
            pltpu.VMEM((1, 1, 128), F32),
            pltpu.VMEM((sizes[0] * sizes[1], 1, 128), F32),
            pltpu.VMEM((1, 1, 128), F32),
            pltpu.VMEM((sizes[2] * 2, 1, 128), F32),
            dma((6,)),
            dma((6,)),
            dma((6,)),
            dma((3,)),
            dma((3,)),
            dma((3, longest)),
            dma((3, longest)),
            dma((3,)),
            dma((3,)),
            dma(()),
            dma(()),
            dma(()),
            dma(()),
            dma(()),
        ],
        compiler_params=pltpu.CompilerParams(
            collective_id=0, has_side_effects=True, vmem_limit_bytes=60 * 1024 * 1024
        ),
    )(
        jnp.transpose(ranges, (2, 0, 1)),
        strengths,
        live,
        pots,
        counts,
        parents,
        turn_counts,
        reach,
        jnp.asarray(card_hots(), BF16),
    )
    return turn_values, total[0, 0]


def solution(mesh):
    sides = {128: (4, 4, 4), 16: (2, 2, 2)}[mesh.devices.size]
    split = Mesh(mesh.devices.reshape(*sides, 2), AXES)
    in_specs = (
        P(NODE, None, "hand"),
        P(NODE, None),
        P(NODE, None),
        P(NODE, None),
        P(NODE),
        P(NODE),
        P(),
        P(None, None, "hand"),
    )
    out_specs = (P(NODE, None, "hand"), P())
    return jax.shard_map(
        functools.partial(local, sides),
        mesh=split,
        in_specs=in_specs,
        out_specs=out_specs,
        check_vma=False,
    )
```

```python
import functools

import jax
import jax.numpy as jnp
import numpy as np
from jax import lax
from jax.experimental import pallas as pl
from jax.experimental.pallas import tpu as pltpu
from jax.sharding import Mesh
from jax.sharding import PartitionSpec as P

AXES = ("node_0", "node_1", "node_2", "hand")
NODE = AXES[:3]
MESH_ID = pl.DeviceIdType.MESH
F32 = jnp.float32
BF16 = jnp.bfloat16

ACT = 8
GROUPS = 8
TACT = 4
LINES = 128
HALF = 663
WIDE = 768
LOCAL = 32
MINE = 16
EARLY = 3
TALL = 672
K_TILES = ((0, 256), (256, 256), (512, 160))
J_BLOCKS = tuple((b * 128, min(128, HALF - b * 128)) for b in range(6))


def card_hots():
    first, second = np.triu_indices(52, 1)
    hots = np.zeros((4, WIDE, 64), np.float32)
    for half in range(2):
        for h in range(HALF):
            cards = [first[half * HALF + h], second[half * HALF + h]]
            hots[half, h, cards] = 1.0
            hots[2 + half, h, cards] = -1.0
            hots[2 + half, h, 52] = 1.0
        hots[half, :, 52] = 1.0
    return hots


def tall(row, rows):
    width = row.shape[1]
    block = jnp.broadcast_to(row, (16, width)).astype(BF16)
    return jnp.broadcast_to(block[None], (rows // 16, 16, width)).reshape(rows, width)


def turned(row):
    return jnp.broadcast_to(row, (128, 128)).T


def merged(parts, reduce):
    row = lax.broadcasted_iota(jnp.int32, (8, 128), 0)
    for bit in (1, 2, 4):
        low = (row & bit) == 0
        pairs = []
        for one, two in zip(parts[::2], parts[1::2]):
            kept = jnp.where(low, one, two)
            moved = pltpu.roll(jnp.where(low, two, one), 8 - bit, axis=0)
            pairs.append(reduce(kept, moved))
        parts = pairs
    return parts[0]


def kernel(
    sizes,
    ranges,
    strengths_in,
    live_in,
    pots_in,
    counts,
    parents,
    turn_counts,
    reach,
    hots_in,
    turn_out,
    total_out,
    strengths,
    live,
    pots,
    hots,
    raw,
    by_node,
    masked,
    s_rows,
    live_rows,
    pot_rows,
    s_columns,
    bounds,
    pot_columns,
    partial,
    hot,
    gathered,
    outgoing,
    keys,
    sums,
    arrived,
    my_reach,
    my_part,
    parts_got,
    own_sem,
    other_sem,
    ranges_send,
    line_recv,
    line_send,
    key_recv,
    key_send,
    plane_recv,
    plane_send,
    reach_sem,
    part_recv,
    part_send,
    small_sem,
):
    place = [lax.axis_index(name) for name in NODE]
    core = lax.axis_index("hand")
    far = 1 - core
    turn = (place[0] * sizes[1] + place[1]) * sizes[2] + place[2]
    planes = ((1, 2), (0, 2), (0, 1))

    def at(where, which):
        return (where[0], where[1], where[2], which)

    def along(axis, step):
        where = list(place)
        where[axis] = lax.rem(place[axis] + step, sizes[axis])
        return where

    def plane_size(axis):
        high, low = planes[axis]
        return sizes[high] * sizes[low]

    def plane_mine(axis):
        high, low = planes[axis]
        return place[high] * sizes[low] + place[low]

    def in_plane(axis, slot):
        high, low = planes[axis]
        where = list(place)
        where[high] = slot // sizes[low]
        where[low] = lax.rem(slot, sizes[low])
        return where

    shifts = [
        [lax.rem(place[axis] + step, sizes[axis]) for step in range(sizes[axis])]
        for axis in range(3)
    ]
    peers = [
        (shifts[0][i], shifts[1][j], shifts[2][k], which)
        for i in range(sizes[0])
        for j in range(sizes[1])
        for k in range(sizes[2])
        for which in (core, far)
    ][1:]

    first = core * MINE
    def fetch(block):
        start, width = J_BLOCKS[block]
        return pltpu.make_async_copy(
            ranges.at[pl.ds(start, width), pl.ds(pl.multiple_of(first, MINE), MINE)],
            raw.at[0, pl.ds(start, width)],
            own_sem.at[block],
        )

    def exchange(block):
        start, width = J_BLOCKS[block]
        theirs = pl.ds(pl.multiple_of(far * MINE, MINE), MINE)
        return pltpu.make_async_remote_copy(
            src_ref=ranges.at[pl.ds(start, width), theirs],
            dst_ref=raw.at[1, pl.ds(start, width)],
            send_sem=ranges_send.at[block],
            recv_sem=other_sem.at[block],
            device_id=at(place, far),
            device_id_type=MESH_ID,
        )

    rows = pl.ds(pl.multiple_of(first, MINE), MINE)
    small = [
        pltpu.make_async_copy(source, target, small_sem.at[i])
        for i, (source, target) in enumerate(
            (
                (strengths_in.at[rows], strengths),
                (live_in.at[rows], live),
                (pots_in.at[rows], pots),
                (hots_in, hots),
            )
        )
    ]
    for copy in small:
        copy.start()
    for block in range(6):
        fetch(block).start()
    pltpu.make_async_copy(reach.at[turn], my_reach, reach_sem).start()

    barrier = pltpu.get_barrier_semaphore()
    for peer in peers:
        pl.semaphore_signal(barrier, inc=1, device_id=peer, device_id_type=MESH_ID)

    for copy in small:
        copy.wait()
    s_rows[...] = jnp.full_like(s_rows, -1000.0)
    live_rows[...] = jnp.zeros_like(live_rows)
    for source, target, shift in ((strengths, s_rows, 200.0), (live, live_rows, 0.0)):
        low = source[:, 0:HALF].astype(F32) - shift
        high = source[:, HALF : 2 * HALF].astype(F32) - shift
        mine, theirs = jnp.where(core == 0, low, high), jnp.where(core == 0, high, low)
        for n in range(MINE):
            target[0, n, :, 0:HALF] = mine[n : n + 1]
            target[1, n, :, 0:HALF] = theirs[n : n + 1]
    my_pots = pots[...]
    for n in range(MINE):
        pot_rows[n] = my_pots[n : n + 1]

    def build(group, _):
        lanes = pl.ds(pl.multiple_of(group * 256, 256), 256)
        for j_half, j_core in enumerate((core, far)):
            for i_half, i_core in enumerate((core, far)):
                free = lax.dot_general(
                    hots[j_core, 0:TALL, :],
                    hots[2 + i_core, lanes, :],
                    (((1,), (1,)), ((), ())),
                    preferred_element_type=F32,
                ).astype(BF16)
                for side in range(2):
                    part = free[:, side * 128 : side * 128 + 128]
                    zero = jnp.zeros_like(part)
                    where = i_half * 6 + group * 2 + side
                    bounds[j_half, where, 0, 0:TALL, :] = jnp.maximum(part, zero)
                    bounds[j_half, where, 1, 0:TALL, :] = jnp.minimum(-part, zero)
        return 0

    lax.fori_loop(0, 3, build, 0)

    def swap(half, wait):
        for block in range(6):
            wait(block)

        def one(block, _):
            rows = pl.ds(pl.multiple_of(block * 128, 128), 128)
            by_node[half, :, rows, :] = jnp.swapaxes(raw[half, rows], 0, 1)
            return 0

        lax.fori_loop(0, 5, one, 0)
        by_node[half, :, 640:TALL, :] = jnp.swapaxes(raw[half, 640:TALL], 0, 1)

    lane = lax.broadcasted_iota(jnp.int32, (LINES, 128), 1)
    action = lax.rem(lax.broadcasted_iota(jnp.int32, (LINES, 128), 0), ACT)

    def prepare(half, n, slot):
        for block in range(6):
            lanes = pl.ds(block * 128, 128)
            flags = tall(live_rows[half, n, :, lanes], LINES)
            if block < 5:
                s_columns[slot, lanes, :] = turned(s_rows[half, n, :, lanes].astype(BF16))
                masked[slot, block] = by_node[half, n, lanes, :].T * flags
            else:
                column = turned(s_rows[half, n, :, lanes].astype(BF16))
                s_columns[slot, 640:TALL, :] = column[: TALL - 640]
                last = by_node[half, n, 640:TALL, :]
                last = jnp.concatenate([last, jnp.zeros((96, 128), BF16)], axis=0).T
                last = (last * flags).astype(F32)
                bar = jnp.where(action < counts[first + n], 0.0, -1024.0)
                bar = jnp.where(lane == HALF - 640, bar, 0.0)
                masked[slot, block] = jnp.where(lane < HALF - 640, last, bar).astype(BF16)

    def product(half, n, slot, tile):
        added = None
        for step, (start, height) in enumerate(K_TILES):
            inner = pl.ds(start, height)
            column = s_columns[slot, inner, :]
            signs = []
            for side in range(4):
                where = tile * 4 + side
                lanes = pl.ds((where % 6) * 128, 128)
                gap = tall(s_rows[where // 6, n, :, lanes], height) - column
                signs.append(
                    jnp.minimum(
                        jnp.maximum(gap, bounds[half, where, 1, inner, :]),
                        bounds[half, where, 0, inner, :],
                    )
                )
            left = jnp.concatenate([masked[slot, 2 * step], masked[slot, 2 * step + 1]], axis=1)
            term = jnp.dot(
                left[:, :height],
                jnp.concatenate(signs, axis=1),
                preferred_element_type=F32,
            )
            added = term if added is None else added + term
        return added

    def own_half(pair, _):
        for slot in range(2):
            prepare(0, 2 * pair + slot, slot)
        for slot in range(2):
            n = 2 * pair + slot
            for tile in range(3):
                partial[n, :, pl.ds(tile * 512, 512)] = product(0, n, slot, tile)
        return 0

    swap(0, lambda block: fetch(block).wait())
    lax.fori_loop(0, EARLY, own_half, 0)
    pl.semaphore_wait(barrier, len(peers))
    for block in range(6):
        exchange(block).start()

    lane_row = lax.broadcasted_iota(jnp.int32, (1, 128), 1)
    spread = jnp.zeros((1, 128), jnp.int32)
    for n in range(LOCAL):
        spread = jnp.where(lane_row // 4 == n, parents[n], spread)
    key_row = (spread * 4 + lax.rem(lane_row, 4)).astype(F32)

    def key_copy(axis, step):
        return pltpu.make_async_remote_copy(
            src_ref=keys.at[axis, 0],
            dst_ref=keys.at[axis, sizes[axis] - step],
            send_sem=key_send.at[axis, step],
            recv_sem=key_recv.at[axis, sizes[axis] - step],
            device_id=at(along(axis, step), core),
            device_id_type=MESH_ID,
        )

    for axis in range(3):
        keys[axis, 0] = key_row
        for step in range(1, sizes[axis]):
            key_copy(axis, step).start()

    lax.fori_loop(EARLY, MINE // 2, own_half, 0)
    swap(1, lambda block: exchange(block).wait_recv())

    my_block = core * (MINE * 4)

    def river_copies(batch):
        copies = []
        from_rows = pl.ds(pl.multiple_of(batch * 8, 8), 8)
        mine = pl.ds(pl.multiple_of(my_block + batch * 8, 8), 8)
        for axis in range(3):
            send, recv = line_send.at[axis], line_recv.at[axis]
            for step in range(1, sizes[axis]):
                base = (sizes[axis] - step) * 128
                there = pl.ds(pl.multiple_of(base + my_block + batch * 8, 8), 8)
                for source, which in (
                    (gathered.at[axis, mine], core),
                    (outgoing.at[axis, from_rows], far),
                ):
                    copies.append(
                        pltpu.make_async_remote_copy(
                            src_ref=source,
                            dst_ref=gathered.at[axis, there],
                            send_sem=send,
                            recv_sem=recv,
                            device_id=at(along(axis, step), which),
                            device_id_type=MESH_ID,
                        )
                    )
            copies.append(
                pltpu.make_async_remote_copy(
                    src_ref=outgoing.at[axis, from_rows],
                    dst_ref=gathered.at[axis, mine],
                    send_sem=send,
                    recv_sem=recv,
                    device_id=at(place, far),
                    device_id_type=MESH_ID,
                )
            )
        return copies

    def two_nodes(batch, _):
        for slot in range(2):
            n = 2 * batch + slot
            prepare(1, n, slot)
            pot_columns[slot] = turned(pot_rows[n])
        rivers = [[] for _ in range(6)]
        for tile in range(3):
            for slot in range(2):
                n = 2 * batch + slot
                values = product(1, n, slot, tile) + partial[n, :, pl.ds(tile * 512, 512)]
                for pair in range(2):
                    chunk = tile * 2 + pair
                    for player in range(2):
                        for side in range(2):
                            start = (chunk % 3) * 256 + side * 128
                            parts = []
                            for g in range(GROUPS):
                                row = (player * GROUPS + g) * ACT
                                lane0 = pair * 256 + side * 128
                                part = values[row : row + 8, lane0 : lane0 + 128]
                                parts.append(part * pot_columns[slot, row : row + 8, :])
                            best = merged(parts, jnp.maximum)
                            flags = live_rows[chunk // 3, n, :, pl.ds(start, 128)]
                            rivers[chunk].append(best * flags)
        for chunk in range(6):
            block = merged(rivers[chunk], jnp.add)
            if chunk < 3:
                gathered[chunk, pl.ds(pl.multiple_of(my_block + batch * 8, 8), 8), :] = block
            else:
                outgoing[chunk - 3, pl.ds(pl.multiple_of(batch * 8, 8), 8), :] = block
        for copy in river_copies(batch):
            copy.start()
        return 0

    lax.fori_loop(0, MINE // 2, two_nodes, 0)

    for axis in range(3):
        for step in range(1, sizes[axis]):
            key_copy(axis, step).wait_recv()

    for axis in range(3):
        count = plane_size(axis)
        q = lax.broadcasted_iota(jnp.int32, (count * 16, 128), 0)
        there = in_plane(axis, q // 16)
        owner = (there[0] * sizes[1] + there[1]) * sizes[2] + there[2]
        wanted = (owner * (TACT * 4) + lax.rem(q, 16)).astype(F32)
        for e in range(sizes[axis]):
            hit = jnp.where(wanted == keys[axis, e], 1.0, 0.0).astype(BF16)
            hot[axis, e, 0 : count * 16, :] = hit

    for axis in range(3):
        count = plane_size(axis)
        lines = sizes[axis] * 128
        blocks = (sizes[axis] - 1) * 128 + 64
        whole = gathered.at[axis, pl.ds(0, blocks)]
        pltpu.make_async_copy(whole, whole, line_recv.at[axis]).wait()
        rows_in = gathered[axis, pl.ds(0, lines), :]
        upper = rows_in.astype(BF16)
        lower = (rows_in - upper.astype(F32)).astype(BF16)
        left = jnp.concatenate(
            [hot[axis, e, 0 : count * 16, :] for e in range(sizes[axis])], axis=1
        )
        both = jnp.dot(left, upper, preferred_element_type=F32) + jnp.dot(
            left, lower, preferred_element_type=F32
        )
        sums[axis, pl.ds(0, count * 16), :] = both
        mine = plane_mine(axis)
        here = pl.ds(pl.multiple_of(mine * 16, 16), 16)
        for step in range(1, count):
            slot = lax.rem(mine + step, count)
            part = pl.ds(pl.multiple_of(slot * 16, 16), 16)
            pltpu.make_async_remote_copy(
                src_ref=sums.at[axis, part],
                dst_ref=arrived.at[axis, here],
                send_sem=plane_send.at[axis],
                recv_sem=plane_recv.at[axis],
                device_id=at(in_plane(axis, slot), core),
                device_id_type=MESH_ID,
            ).start()
        arrived[axis, here, :] = sums[axis, here, :]

    pltpu.make_async_copy(reach.at[turn], my_reach, reach_sem).wait()
    legal = turn_counts[turn]
    spot = lax.broadcasted_iota(jnp.int32, (1, 128), 1)
    weighed = jnp.zeros((1, 128), F32)
    for axis in range(3):
        count = plane_size(axis)
        whole = arrived.at[axis, pl.ds(0, (count - 1) * 16)]
        pltpu.make_async_copy(whole, whole, plane_recv.at[axis]).wait()
        total = arrived[axis, pl.ds(0, count * 16), :].reshape(count, 16, 128).sum(axis=0)
        best = total[0:4]
        for a in range(1, TACT):
            best = jnp.maximum(best, jnp.where(a < legal, total[4 * a : 4 * a + 4], -1e30))
        for player in range(2):
            for side in range(2):
                piece = best[player * 2 + side : player * 2 + side + 1]
                start = axis * 256 + side * 128
                width = min(128, HALF - start)
                lanes = pl.ds(start, width)
                turn_out[0, pl.ds(player, 1), lanes] = piece[:, :width]
                part = piece[:, :width] * my_reach[pl.ds(player, 1), lanes]
                if width == 128:
                    weighed = weighed + part
                else:
                    weighed = weighed + jnp.where(
                        spot == 0, jnp.sum(part, axis=1, keepdims=True), 0.0
                    )

    slot = turn * 2 + core
    my_part[0] = weighed
    parts_got[slot] = weighed
    for peer in peers:
        pltpu.make_async_remote_copy(
            src_ref=my_part.at[0],
            dst_ref=parts_got.at[slot],
            send_sem=part_send,
            recv_sem=part_recv,
            device_id=peer,
            device_id_type=MESH_ID,
        ).start()

    for block in range(6):
        exchange(block).wait_send()
    for axis in range(3):
        for step in range(1, sizes[axis]):
            key_copy(axis, step).wait_send()
        sent = gathered.at[axis, pl.ds(0, (sizes[axis] - 1) * 64)]
        for _ in range(2):
            pltpu.make_async_copy(sent, sent, line_send.at[axis]).wait()
        sent = gathered.at[axis, pl.ds(0, 64)]
        pltpu.make_async_copy(sent, sent, line_send.at[axis]).wait()
        sent = arrived.at[axis, pl.ds(0, (plane_size(axis) - 1) * 16)]
        pltpu.make_async_copy(sent, sent, plane_send.at[axis]).wait()
    sent = parts_got.at[pl.ds(0, len(peers))]
    pltpu.make_async_copy(sent, sent, part_send).wait()
    pltpu.make_async_copy(sent, sent, part_recv).wait()
    total_out[0, 0] = jnp.sum(parts_got[...].sum(axis=0))


def local(sizes, ranges, strengths, live, pots, counts, parents, turn_counts, reach):
    dma = pltpu.SemaphoreType.DMA
    longest = max(sizes)
    widest = max(sizes[0] * sizes[1], sizes[1] * sizes[2], sizes[0] * sizes[2])
    vmem = pl.BlockSpec(memory_space=pltpu.VMEM)
    smem = pl.BlockSpec(memory_space=pltpu.SMEM)
    hbm = pl.BlockSpec(memory_space=pl.ANY)
    turn_values, total = pl.pallas_call(
        functools.partial(kernel, sizes),
        out_shape=(
            jax.ShapeDtypeStruct((1, 2, HALF), F32),
            jax.ShapeDtypeStruct((1, 1), F32),
        ),
        in_specs=[hbm, hbm, hbm, hbm, smem, smem, smem, hbm, hbm],
        out_specs=(vmem, smem),
        scratch_shapes=[
            pltpu.VMEM((MINE, 2 * HALF), jnp.int32),
            pltpu.VMEM((MINE, 2 * HALF), jnp.int32),
            pltpu.VMEM((MINE, LINES), F32),
            pltpu.VMEM((4, WIDE, 64), BF16),
            pltpu.VMEM((2, TALL, MINE, LINES), BF16),
            pltpu.VMEM((2, MINE, TALL, LINES), BF16),
            pltpu.VMEM((2, 6, LINES, 128), BF16),
            pltpu.VMEM((2, MINE, 1, WIDE), F32),
            pltpu.VMEM((2, MINE, 1, WIDE), F32),
            pltpu.VMEM((MINE, 1, LINES), F32),
            pltpu.VMEM((2, TALL, 128), BF16),
            pltpu.VMEM((2, 12, 2, TALL + 16, 128), BF16),
            pltpu.VMEM((2, LINES, 128), F32),
            pltpu.VMEM((MINE, LINES, 2 * WIDE), F32),
            pltpu.VMEM((3, longest, widest * 16, 128), BF16),
            pltpu.VMEM((3, longest * 128, 128), F32),
            pltpu.VMEM((3, 64, 128), F32),
            pltpu.VMEM((3, longest, 1, 128), F32),
            pltpu.VMEM((3, widest * 16, 128), F32),
            pltpu.VMEM((3, widest * 16, 128), F32),
            pltpu.VMEM((2, HALF), F32),
            pltpu.VMEM((1, 1, 128), F32),
            pltpu.VMEM((sizes[0] * sizes[1] * sizes[2] * 2, 1, 128), F32),
            dma((6,)),
            dma((6,)),
            dma((6,)),
            dma((3,)),
            dma((3,)),
            dma((3, longest)),
            dma((3, longest)),
            dma((3,)),
            dma((3,)),
            dma(()),
            dma(()),
            dma(()),
            dma((4,)),
        ],
        compiler_params=pltpu.CompilerParams(
            collective_id=0,
            has_side_effects=True,
            vmem_limit_bytes=62 * 1024 * 1024,
        ),
    )(
        jnp.transpose(ranges, (2, 0, 1)),
        strengths,
        live,
        pots,
        counts,
        parents,
        turn_counts,
        reach,
        jnp.asarray(card_hots(), BF16),
    )
    return turn_values, total[0, 0]


def solution(mesh):
    sides = {128: (4, 4, 4), 16: (2, 2, 2)}[mesh.devices.size]
    split = Mesh(mesh.devices.reshape(*sides, 2), AXES)
    in_specs = (
        P(NODE, None, "hand"),
        P(NODE, None),
        P(NODE, None),
        P(NODE, None),
        P(NODE),
        P(NODE),
        P(),
        P(None, None, "hand"),
    )
    out_specs = (P(NODE, None, "hand"), P())
    return jax.shard_map(
        functools.partial(local, sides),
        mesh=split,
        in_specs=in_specs,
        out_specs=out_specs,
        check_vma=False,
    )
```

```python
import functools

import jax
import jax.numpy as jnp
import numpy as np
from jax import lax
from jax.experimental import pallas as pl
from jax.experimental.pallas import tpu as pltpu
from jax.sharding import Mesh
from jax.sharding import PartitionSpec as P

AXES = ("node_0", "node_1", "node_2", "hand")
NODE = AXES[:3]
MESH_ID = pl.DeviceIdType.MESH
F32 = jnp.float32
BF16 = jnp.bfloat16

ACT = 8
GROUPS = 8
TACT = 4
LINES = 128
HALF = 663
WIDE = 768
LOCAL = 32
MINE = 16
EARLY = 1
TALL = 672
K_TILES = ((0, 256), (256, 256), (512, 160))
J_BLOCKS = tuple((b * 128, min(128, HALF - b * 128)) for b in range(6))


def card_hots():
    first, second = np.triu_indices(52, 1)
    hots = np.zeros((4, WIDE, 64), np.float32)
    for half in range(2):
        for h in range(HALF):
            cards = [first[half * HALF + h], second[half * HALF + h]]
            hots[half, h, cards] = 1.0
            hots[2 + half, h, cards] = -1.0
            hots[2 + half, h, 52] = 1.0
        hots[half, :, 52] = 1.0
    return hots


def tall(row, rows):
    width = row.shape[1]
    block = jnp.broadcast_to(row, (16, width)).astype(BF16)
    return jnp.broadcast_to(block[None], (rows // 16, 16, width)).reshape(rows, width)


def turned(row):
    return jnp.broadcast_to(row, (128, 128)).T


def merged(parts, reduce):
    row = lax.broadcasted_iota(jnp.int32, (8, 128), 0)
    for bit in (1, 2, 4):
        low = (row & bit) == 0
        pairs = []
        for one, two in zip(parts[::2], parts[1::2]):
            kept = jnp.where(low, one, two)
            moved = pltpu.roll(jnp.where(low, two, one), 8 - bit, axis=0)
            pairs.append(reduce(kept, moved))
        parts = pairs
    return parts[0]


def kernel(
    sizes,
    ranges,
    strengths_in,
    live_in,
    pots_in,
    counts,
    parents,
    turn_counts,
    reach,
    hots_in,
    turn_out,
    total_out,
    strengths,
    live,
    pots,
    hots,
    raw,
    by_node,
    masked,
    s_rows,
    live_rows,
    pot_rows,
    s_columns,
    bounds,
    pot_columns,
    partial,
    hot,
    gathered,
    outgoing,
    keys,
    sums,
    arrived,
    my_reach,
    my_part,
    parts_got,
    own_sem,
    other_sem,
    ranges_send,
    line_recv,
    line_send,
    key_recv,
    key_send,
    plane_recv,
    plane_send,
    reach_sem,
    part_recv,
    part_send,
    small_sem,
):
    place = [lax.axis_index(name) for name in NODE]
    core = lax.axis_index("hand")
    far = 1 - core
    turn = (place[0] * sizes[1] + place[1]) * sizes[2] + place[2]
    planes = ((1, 2), (0, 2), (0, 1))

    def at(where, which):
        return (where[0], where[1], where[2], which)

    def along(axis, step):
        where = list(place)
        where[axis] = lax.rem(place[axis] + step, sizes[axis])
        return where

    def plane_size(axis):
        high, low = planes[axis]
        return sizes[high] * sizes[low]

    def plane_mine(axis):
        high, low = planes[axis]
        return place[high] * sizes[low] + place[low]

    def in_plane(axis, slot):
        high, low = planes[axis]
        where = list(place)
        where[high] = slot // sizes[low]
        where[low] = lax.rem(slot, sizes[low])
        return where

    shifts = [
        [lax.rem(place[axis] + step, sizes[axis]) for step in range(sizes[axis])]
        for axis in range(3)
    ]
    peers = [
        (shifts[0][i], shifts[1][j], shifts[2][k], which)
        for i in range(sizes[0])
        for j in range(sizes[1])
        for k in range(sizes[2])
        for which in (core, far)
    ][1:]

    first = core * MINE
    def fetch(block):
        start, width = J_BLOCKS[block]
        return pltpu.make_async_copy(
            ranges.at[pl.ds(start, width), pl.ds(pl.multiple_of(first, MINE), MINE)],
            raw.at[0, pl.ds(start, width)],
            own_sem.at[block],
        )

    def exchange(block):
        start, width = J_BLOCKS[block]
        theirs = pl.ds(pl.multiple_of(far * MINE, MINE), MINE)
        return pltpu.make_async_remote_copy(
            src_ref=ranges.at[pl.ds(start, width), theirs],
            dst_ref=raw.at[1, pl.ds(start, width)],
            send_sem=ranges_send.at[block],
            recv_sem=other_sem.at[block],
            device_id=at(place, far),
            device_id_type=MESH_ID,
        )

    rows = pl.ds(pl.multiple_of(first, MINE), MINE)
    small = [
        pltpu.make_async_copy(source, target, small_sem.at[i])
        for i, (source, target) in enumerate(
            (
                (strengths_in.at[rows], strengths),
                (live_in.at[rows], live),
                (pots_in.at[rows], pots),
                (hots_in, hots),
            )
        )
    ]
    for copy in small:
        copy.start()
    for block in range(6):
        fetch(block).start()
    pltpu.make_async_copy(reach.at[turn], my_reach, reach_sem).start()

    barrier = pltpu.get_barrier_semaphore()
    for peer in peers:
        pl.semaphore_signal(barrier, inc=1, device_id=peer, device_id_type=MESH_ID)

    for copy in small:
        copy.wait()
    s_rows[...] = jnp.full_like(s_rows, -1000.0)
    live_rows[...] = jnp.zeros_like(live_rows)
    for source, target, shift in ((strengths, s_rows, 200.0), (live, live_rows, 0.0)):
        low = source[:, 0:HALF].astype(F32) - shift
        high = source[:, HALF : 2 * HALF].astype(F32) - shift
        mine, theirs = jnp.where(core == 0, low, high), jnp.where(core == 0, high, low)
        for n in range(MINE):
            target[0, n, :, 0:HALF] = mine[n : n + 1]
            target[1, n, :, 0:HALF] = theirs[n : n + 1]
    my_pots = pots[...]
    for n in range(MINE):
        pot_rows[n] = my_pots[n : n + 1]

    def build(group, _):
        lanes = pl.ds(pl.multiple_of(group * 256, 256), 256)
        for j_half, j_core in enumerate((core, far)):
            for i_half, i_core in enumerate((core, far)):
                free = lax.dot_general(
                    hots[j_core, 0:TALL, :],
                    hots[2 + i_core, lanes, :],
                    (((1,), (1,)), ((), ())),
                    preferred_element_type=F32,
                ).astype(BF16)
                for side in range(2):
                    part = free[:, side * 128 : side * 128 + 128]
                    zero = jnp.zeros_like(part)
                    where = i_half * 6 + group * 2 + side
                    bounds[j_half, where, 0, 0:TALL, :] = jnp.maximum(part, zero)
                    bounds[j_half, where, 1, 0:TALL, :] = jnp.minimum(-part, zero)
        return 0

    lax.fori_loop(0, 3, build, 0)

    def swap(half, wait):
        for block in range(6):
            wait(block)

        def one(block, _):
            for part in range(4):
                rows = pl.ds(pl.multiple_of(block * 128 + part * 32, 32), 32)
                by_node[half, :, rows, :] = jnp.swapaxes(raw[half, rows], 0, 1)
            return 0

        lax.fori_loop(0, 5, one, 0)
        by_node[half, :, 640:TALL, :] = jnp.swapaxes(raw[half, 640:TALL], 0, 1)

    lane = lax.broadcasted_iota(jnp.int32, (LINES, 128), 1)
    action = lax.rem(lax.broadcasted_iota(jnp.int32, (LINES, 128), 0), ACT)

    def prepare(half, n, slot):
        if half == 1:
            pot_columns[slot] = turned(pot_rows[n])
        for block in range(6):
            lanes = pl.ds(block * 128, 128)
            flags = tall(live_rows[half, n, :, lanes], LINES)
            if block < 5:
                s_columns[slot, lanes, :] = turned(s_rows[half, n, :, lanes].astype(BF16))
                masked[slot, block] = by_node[half, n, lanes, :].T * flags
            else:
                column = turned(s_rows[half, n, :, lanes].astype(BF16))
                s_columns[slot, 640:TALL, :] = column[: TALL - 640]
                last = by_node[half, n, 640:TALL, :]
                last = jnp.concatenate([last, jnp.zeros((96, 128), BF16)], axis=0).T
                last = (last * flags).astype(F32)
                bar = jnp.where(action < counts[first + n], 0.0, -1024.0)
                bar = jnp.where(lane == HALF - 640, bar, 0.0)
                masked[slot, block] = jnp.where(lane < HALF - 640, last, bar).astype(BF16)

    def product(half, n, slot, tile):
        added = None
        for step, (start, height) in enumerate(K_TILES):
            inner = pl.ds(start, height)
            column = s_columns[slot, inner, :]
            signs = []
            for side in range(4):
                where = tile * 4 + side
                lanes = pl.ds((where % 6) * 128, 128)
                gap = tall(s_rows[where // 6, n, :, lanes], height) - column
                signs.append(
                    jnp.minimum(
                        jnp.maximum(gap, bounds[half, where, 1, inner, :]),
                        bounds[half, where, 0, inner, :],
                    )
                )
            left = jnp.concatenate([masked[slot, 2 * step], masked[slot, 2 * step + 1]], axis=1)
            term = jnp.dot(
                left[:, :height],
                jnp.concatenate(signs, axis=1),
                preferred_element_type=F32,
            )
            added = term if added is None else added + term
        return added

    def ahead(half, base, slots):
        for k, slot in enumerate(slots):
            last = base + k if isinstance(base, int) else jnp.minimum(base + k, MINE - 1)
            prepare(half, last, slot)

    def own_half(group, _):
        for part in range(2):
            ahead(0, 4 * group + 2 * part + 2, (2, 3) if part == 0 else (0, 1))
            for k in range(2):
                slot = 2 * part + k
                n = 4 * group + slot
                for tile in range(3):
                    partial[n, :, pl.ds(tile * 512, 512)] = product(0, n, slot, tile)
        return 0

    swap(0, lambda block: fetch(block).wait())
    ahead(0, 0, (0, 1))
    lax.fori_loop(0, EARLY, own_half, 0)
    pl.semaphore_wait(barrier, len(peers))
    for block in range(6):
        exchange(block).start()

    lane_row = lax.broadcasted_iota(jnp.int32, (1, 128), 1)
    spread = jnp.zeros((1, 128), jnp.int32)
    for n in range(LOCAL):
        spread = jnp.where(lane_row // 4 == n, parents[n], spread)
    key_row = (spread * 4 + lax.rem(lane_row, 4)).astype(F32)

    def key_copy(axis, step):
        return pltpu.make_async_remote_copy(
            src_ref=keys.at[axis, 0],
            dst_ref=keys.at[axis, sizes[axis] - step],
            send_sem=key_send.at[axis, step],
            recv_sem=key_recv.at[axis, sizes[axis] - step],
            device_id=at(along(axis, step), core),
            device_id_type=MESH_ID,
        )

    for axis in range(3):
        keys[axis, 0] = key_row
        for step in range(1, sizes[axis]):
            key_copy(axis, step).start()

    lax.fori_loop(EARLY, MINE // 4, own_half, 0)
    swap(1, lambda block: exchange(block).wait_recv())
    ahead(1, 0, (0, 1))

    my_block = core * (MINE * 4)

    def river_copies(group):
        copies = []
        from_rows = pl.ds(pl.multiple_of(group * 16, 16), 16)
        mine = pl.ds(pl.multiple_of(my_block + group * 16, 16), 16)
        for axis in range(3):
            send, recv = line_send.at[axis], line_recv.at[axis]
            for step in range(1, sizes[axis]):
                base = (sizes[axis] - step) * 128
                there = pl.ds(pl.multiple_of(base + my_block + group * 16, 16), 16)
                for source, which in (
                    (gathered.at[axis, mine], core),
                    (outgoing.at[axis, from_rows], far),
                ):
                    copies.append(
                        pltpu.make_async_remote_copy(
                            src_ref=source,
                            dst_ref=gathered.at[axis, there],
                            send_sem=send,
                            recv_sem=recv,
                            device_id=at(along(axis, step), which),
                            device_id_type=MESH_ID,
                        )
                    )
            copies.append(
                pltpu.make_async_remote_copy(
                    src_ref=outgoing.at[axis, from_rows],
                    dst_ref=gathered.at[axis, mine],
                    send_sem=send,
                    recv_sem=recv,
                    device_id=at(place, far),
                    device_id_type=MESH_ID,
                )
            )
        return copies

    def two_nodes(batch, part):
        ahead(1, 2 * batch + 2, (2, 3) if part == 0 else (0, 1))
        rivers = [[] for _ in range(6)]
        for tile in range(3):
            for slot in (2 * part, 2 * part + 1):
                n = 2 * batch + slot - 2 * part
                values = product(1, n, slot, tile) + partial[n, :, pl.ds(tile * 512, 512)]
                for pair in range(2):
                    chunk = tile * 2 + pair
                    for player in range(2):
                        for side in range(2):
                            start = (chunk % 3) * 256 + side * 128
                            parts = []
                            for g in range(GROUPS):
                                row = (player * GROUPS + g) * ACT
                                lane0 = pair * 256 + side * 128
                                piece = values[row : row + 8, lane0 : lane0 + 128]
                                parts.append(piece * pot_columns[slot, row : row + 8, :])
                            best = merged(parts, jnp.maximum)
                            flags = live_rows[chunk // 3, n, :, pl.ds(start, 128)]
                            rivers[chunk].append(best * flags)
        for chunk in range(6):
            block = merged(rivers[chunk], jnp.add)
            if chunk < 3:
                gathered[chunk, pl.ds(pl.multiple_of(my_block + batch * 8, 8), 8), :] = block
            else:
                outgoing[chunk - 3, pl.ds(pl.multiple_of(batch * 8, 8), 8), :] = block

    def four_nodes(group, _):
        two_nodes(2 * group, 0)
        two_nodes(2 * group + 1, 1)
        for copy in river_copies(group):
            copy.start()
        return 0

    lax.fori_loop(0, MINE // 4, four_nodes, 0)

    for axis in range(3):
        for step in range(1, sizes[axis]):
            key_copy(axis, step).wait_recv()

    for axis in range(3):
        count = plane_size(axis)
        q = lax.broadcasted_iota(jnp.int32, (count * 16, 128), 0)
        there = in_plane(axis, q // 16)
        owner = (there[0] * sizes[1] + there[1]) * sizes[2] + there[2]
        wanted = (owner * (TACT * 4) + lax.rem(q, 16)).astype(F32)
        for e in range(sizes[axis]):
            hit = jnp.where(wanted == keys[axis, e], 1.0, 0.0).astype(BF16)
            hot[axis, e, 0 : count * 16, :] = hit

    for axis in range(3):
        count = plane_size(axis)
        lines = sizes[axis] * 128
        blocks = (sizes[axis] - 1) * 128 + 64
        whole = gathered.at[axis, pl.ds(0, blocks)]
        pltpu.make_async_copy(whole, whole, line_recv.at[axis]).wait()
        rows_in = gathered[axis, pl.ds(0, lines), :]
        upper = rows_in.astype(BF16)
        lower = (rows_in - upper.astype(F32)).astype(BF16)
        left = jnp.concatenate(
            [hot[axis, e, 0 : count * 16, :] for e in range(sizes[axis])], axis=1
        )
        both = jnp.dot(left, upper, preferred_element_type=F32) + jnp.dot(
            left, lower, preferred_element_type=F32
        )
        sums[axis, pl.ds(0, count * 16), :] = both
        mine = plane_mine(axis)
        here = pl.ds(pl.multiple_of(mine * 16, 16), 16)
        for step in range(1, count):
            slot = lax.rem(mine + step, count)
            part = pl.ds(pl.multiple_of(slot * 16, 16), 16)
            pltpu.make_async_remote_copy(
                src_ref=sums.at[axis, part],
                dst_ref=arrived.at[axis, here],
                send_sem=plane_send.at[axis],
                recv_sem=plane_recv.at[axis],
                device_id=at(in_plane(axis, slot), core),
                device_id_type=MESH_ID,
            ).start()
        arrived[axis, here, :] = sums[axis, here, :]

    pltpu.make_async_copy(reach.at[turn], my_reach, reach_sem).wait()
    legal = turn_counts[turn]
    spot = lax.broadcasted_iota(jnp.int32, (1, 128), 1)
    weighed = jnp.zeros((1, 128), F32)
    for axis in range(3):
        count = plane_size(axis)
        whole = arrived.at[axis, pl.ds(0, (count - 1) * 16)]
        pltpu.make_async_copy(whole, whole, plane_recv.at[axis]).wait()
        total = arrived[axis, pl.ds(0, count * 16), :].reshape(count, 16, 128).sum(axis=0)
        best = total[0:4]
        for a in range(1, TACT):
            best = jnp.maximum(best, jnp.where(a < legal, total[4 * a : 4 * a + 4], -1e30))
        for player in range(2):
            for side in range(2):
                piece = best[player * 2 + side : player * 2 + side + 1]
                start = axis * 256 + side * 128
                width = min(128, HALF - start)
                lanes = pl.ds(start, width)
                turn_out[0, pl.ds(player, 1), lanes] = piece[:, :width]
                part = piece[:, :width] * my_reach[pl.ds(player, 1), lanes]
                if width == 128:
                    weighed = weighed + part
                else:
                    weighed = weighed + jnp.where(
                        spot == 0, jnp.sum(part, axis=1, keepdims=True), 0.0
                    )

    slot = turn * 2 + core
    my_part[0] = weighed
    parts_got[slot] = weighed
    for peer in peers:
        pltpu.make_async_remote_copy(
            src_ref=my_part.at[0],
            dst_ref=parts_got.at[slot],
            send_sem=part_send,
            recv_sem=part_recv,
            device_id=peer,
            device_id_type=MESH_ID,
        ).start()

    for block in range(6):
        exchange(block).wait_send()
    for axis in range(3):
        for step in range(1, sizes[axis]):
            key_copy(axis, step).wait_send()
        sent = gathered.at[axis, pl.ds(0, (sizes[axis] - 1) * 64)]
        for _ in range(2):
            pltpu.make_async_copy(sent, sent, line_send.at[axis]).wait()
        sent = gathered.at[axis, pl.ds(0, 64)]
        pltpu.make_async_copy(sent, sent, line_send.at[axis]).wait()
        sent = arrived.at[axis, pl.ds(0, (plane_size(axis) - 1) * 16)]
        pltpu.make_async_copy(sent, sent, plane_send.at[axis]).wait()
    sent = parts_got.at[pl.ds(0, len(peers))]
    pltpu.make_async_copy(sent, sent, part_send).wait()
    pltpu.make_async_copy(sent, sent, part_recv).wait()
    total_out[0, 0] = jnp.sum(parts_got[...].sum(axis=0))


def local(sizes, ranges, strengths, live, pots, counts, parents, turn_counts, reach):
    dma = pltpu.SemaphoreType.DMA
    longest = max(sizes)
    widest = max(sizes[0] * sizes[1], sizes[1] * sizes[2], sizes[0] * sizes[2])
    vmem = pl.BlockSpec(memory_space=pltpu.VMEM)
    smem = pl.BlockSpec(memory_space=pltpu.SMEM)
    hbm = pl.BlockSpec(memory_space=pl.ANY)
    turn_values, total = pl.pallas_call(
        functools.partial(kernel, sizes),
        out_shape=(
            jax.ShapeDtypeStruct((1, 2, HALF), F32),
            jax.ShapeDtypeStruct((1, 1), F32),
        ),
        in_specs=[hbm, hbm, hbm, hbm, smem, smem, smem, hbm, hbm],
        out_specs=(vmem, smem),
        scratch_shapes=[
            pltpu.VMEM((MINE, 2 * HALF), jnp.int32),
            pltpu.VMEM((MINE, 2 * HALF), jnp.int32),
            pltpu.VMEM((MINE, LINES), F32),
            pltpu.VMEM((4, WIDE, 64), BF16),
            pltpu.VMEM((2, TALL, MINE, LINES), BF16),
            pltpu.VMEM((2, MINE, TALL, LINES), BF16),
            pltpu.VMEM((4, 6, LINES, 128), BF16),
            pltpu.VMEM((2, MINE, 1, WIDE), F32),
            pltpu.VMEM((2, MINE, 1, WIDE), F32),
            pltpu.VMEM((MINE, 1, LINES), F32),
            pltpu.VMEM((4, TALL, 128), BF16),
            pltpu.VMEM((2, 12, 2, TALL + 16, 128), BF16),
            pltpu.VMEM((4, LINES, 128), F32),
            pltpu.VMEM((MINE, LINES, 2 * WIDE), F32),
            pltpu.VMEM((3, longest, widest * 16, 128), BF16),
            pltpu.VMEM((3, longest * 128, 128), F32),
            pltpu.VMEM((3, 64, 128), F32),
            pltpu.VMEM((3, longest, 1, 128), F32),
            pltpu.VMEM((3, widest * 16, 128), F32),
            pltpu.VMEM((3, widest * 16, 128), F32),
            pltpu.VMEM((2, HALF), F32),
            pltpu.VMEM((1, 1, 128), F32),
            pltpu.VMEM((sizes[0] * sizes[1] * sizes[2] * 2, 1, 128), F32),
            dma((6,)),
            dma((6,)),
            dma((6,)),
            dma((3,)),
            dma((3,)),
            dma((3, longest)),
            dma((3, longest)),
            dma((3,)),
            dma((3,)),
            dma(()),
            dma(()),
            dma(()),
            dma((4,)),
        ],
        compiler_params=pltpu.CompilerParams(
            collective_id=0,
            has_side_effects=True,
            vmem_limit_bytes=62 * 1024 * 1024,
        ),
    )(
        jnp.transpose(ranges, (2, 0, 1)),
        strengths,
        live,
        pots,
        counts,
        parents,
        turn_counts,
        reach,
        jnp.asarray(card_hots(), BF16),
    )
    return turn_values, total[0, 0]


def solution(mesh):
    sides = {128: (4, 4, 4), 16: (2, 2, 2)}[mesh.devices.size]
    split = Mesh(mesh.devices.reshape(*sides, 2), AXES)
    in_specs = (
        P(NODE, None, "hand"),
        P(NODE, None),
        P(NODE, None),
        P(NODE, None),
        P(NODE),
        P(NODE),
        P(),
        P(None, None, "hand"),
    )
    out_specs = (P(NODE, None, "hand"), P())
    return jax.shard_map(
        functools.partial(local, sides),
        mesh=split,
        in_specs=in_specs,
        out_specs=out_specs,
        check_vma=False,
    )
```

```python
import functools

import jax
import jax.numpy as jnp
import numpy as np
from jax import lax
from jax.experimental import pallas as pl
from jax.experimental.pallas import tpu as pltpu
from jax.sharding import Mesh
from jax.sharding import PartitionSpec as P

AXES = ("node_0", "node_1", "node_2", "hand")
NODE = AXES[:3]
MESH_ID = pl.DeviceIdType.MESH
F32 = jnp.float32
BF16 = jnp.bfloat16

ACT = 8
GROUPS = 8
TACT = 4
LINES = 128
HALF = 663
WIDE = 768
LOCAL = 32
MINE = 16
EARLY = 1
TALL = 672
K_TILES = ((0, 256), (256, 256), (512, 160))
J_BLOCKS = tuple((b * 128, min(128, HALF - b * 128)) for b in range(6))


def card_hots():
    first, second = np.triu_indices(52, 1)
    hots = np.zeros((4, WIDE, 64), np.float32)
    for half in range(2):
        for h in range(HALF):
            cards = [first[half * HALF + h], second[half * HALF + h]]
            hots[half, h, cards] = 1.0
            hots[2 + half, h, cards] = -1.0
            hots[2 + half, h, 52] = 1.0
        hots[half, :, 52] = 1.0
    return hots


def far_first(sides):
    steps = [step for step in np.ndindex(*sides) if any(step)]
    hops = [sum(min(at, side - at) for at, side in zip(step, sides)) for step in steps]
    return [steps[i] for i in np.argsort(-np.array(hops), kind="stable")]


def tall(row, rows):
    width = row.shape[1]
    block = jnp.broadcast_to(row, (16, width)).astype(BF16)
    return jnp.broadcast_to(block[None], (rows // 16, 16, width)).reshape(rows, width)


def turned(row):
    return jnp.broadcast_to(row, (128, 128)).T


def merged(parts, reduce):
    row = lax.broadcasted_iota(jnp.int32, (8, 128), 0)
    for bit in (1, 2, 4):
        low = (row & bit) == 0
        pairs = []
        for one, two in zip(parts[::2], parts[1::2]):
            kept = jnp.where(low, one, two)
            moved = pltpu.roll(jnp.where(low, two, one), 8 - bit, axis=0)
            pairs.append(reduce(kept, moved))
        parts = pairs
    return parts[0]


def kernel(
    sizes,
    ranges,
    strengths_in,
    live_in,
    pots_in,
    counts,
    parents,
    turn_counts,
    reach,
    hots_in,
    turn_out,
    total_out,
    strengths,
    live,
    pots,
    hots,
    raw,
    by_node,
    masked,
    s_rows,
    live_rows,
    pot_rows,
    s_columns,
    bounds,
    pot_columns,
    partial,
    hot,
    gathered,
    outgoing,
    keys,
    sums,
    arrived,
    my_reach,
    my_part,
    parts_got,
    own_sem,
    other_sem,
    ranges_send,
    line_recv,
    line_send,
    key_recv,
    key_send,
    plane_recv,
    plane_send,
    reach_sem,
    part_recv,
    part_send,
    small_sem,
):
    place = [lax.axis_index(name) for name in NODE]
    core = lax.axis_index("hand")
    far = 1 - core
    turn = (place[0] * sizes[1] + place[1]) * sizes[2] + place[2]
    planes = ((1, 2), (0, 2), (0, 1))

    def at(where, which):
        return (where[0], where[1], where[2], which)

    def along(axis, step):
        where = list(place)
        where[axis] = lax.rem(place[axis] + step, sizes[axis])
        return where

    def plane_size(axis):
        high, low = planes[axis]
        return sizes[high] * sizes[low]

    def plane_mine(axis):
        high, low = planes[axis]
        return place[high] * sizes[low] + place[low]

    def in_plane(axis, slot):
        high, low = planes[axis]
        where = list(place)
        where[high] = slot // sizes[low]
        where[low] = lax.rem(slot, sizes[low])
        return where

    shifts = [
        [lax.rem(place[axis] + step, sizes[axis]) for step in range(sizes[axis])]
        for axis in range(3)
    ]
    peers = [
        (shifts[0][i], shifts[1][j], shifts[2][k], (core, far)[other])
        for i, j, k, other in far_first((*sizes, 2))
    ]

    first = core * MINE
    def fetch(block):
        start, width = J_BLOCKS[block]
        return pltpu.make_async_copy(
            ranges.at[pl.ds(start, width), pl.ds(pl.multiple_of(first, MINE), MINE)],
            raw.at[0, pl.ds(start, width)],
            own_sem.at[block],
        )

    def exchange(block):
        start, width = J_BLOCKS[block]
        theirs = pl.ds(pl.multiple_of(far * MINE, MINE), MINE)
        return pltpu.make_async_remote_copy(
            src_ref=ranges.at[pl.ds(start, width), theirs],
            dst_ref=raw.at[1, pl.ds(start, width)],
            send_sem=ranges_send.at[block],
            recv_sem=other_sem.at[block],
            device_id=at(place, far),
            device_id_type=MESH_ID,
        )

    rows = pl.ds(pl.multiple_of(first, MINE), MINE)
    small = [
        pltpu.make_async_copy(source, target, small_sem.at[i])
        for i, (source, target) in enumerate(
            (
                (strengths_in.at[rows], strengths),
                (live_in.at[rows], live),
                (pots_in.at[rows], pots),
                (hots_in, hots),
            )
        )
    ]
    for copy in small:
        copy.start()
    for block in range(6):
        fetch(block).start()
    pltpu.make_async_copy(reach.at[turn], my_reach, reach_sem).start()

    barrier = pltpu.get_barrier_semaphore()
    for peer in peers:
        pl.semaphore_signal(barrier, inc=1, device_id=peer, device_id_type=MESH_ID)

    for copy in small:
        copy.wait()
    s_rows[...] = jnp.full_like(s_rows, -1000.0)
    live_rows[...] = jnp.zeros_like(live_rows)
    for source, target, shift in ((strengths, s_rows, 200.0), (live, live_rows, 0.0)):
        low = source[:, 0:HALF].astype(F32) - shift
        high = source[:, HALF : 2 * HALF].astype(F32) - shift
        mine, theirs = jnp.where(core == 0, low, high), jnp.where(core == 0, high, low)
        for n in range(MINE):
            target[0, n, :, 0:HALF] = mine[n : n + 1]
            target[1, n, :, 0:HALF] = theirs[n : n + 1]
    my_pots = pots[...]
    for n in range(MINE):
        pot_rows[n] = my_pots[n : n + 1]

    def build(group, _):
        lanes = pl.ds(pl.multiple_of(group * 256, 256), 256)
        for j_half, j_core in enumerate((core, far)):
            for i_half, i_core in enumerate((core, far)):
                free = lax.dot_general(
                    hots[j_core, 0:TALL, :],
                    hots[2 + i_core, lanes, :],
                    (((1,), (1,)), ((), ())),
                    preferred_element_type=F32,
                ).astype(BF16)
                for side in range(2):
                    part = free[:, side * 128 : side * 128 + 128]
                    zero = jnp.zeros_like(part)
                    where = i_half * 6 + group * 2 + side
                    bounds[j_half, where, 0, 0:TALL, :] = jnp.maximum(part, zero)
                    bounds[j_half, where, 1, 0:TALL, :] = jnp.minimum(-part, zero)
        return 0

    lax.fori_loop(0, 3, build, 0)

    def swap(half, wait):
        for block in range(6):
            wait(block)

        def one(block, _):
            for part in range(4):
                rows = pl.ds(pl.multiple_of(block * 128 + part * 32, 32), 32)
                by_node[half, :, rows, :] = jnp.swapaxes(raw[half, rows], 0, 1)
            return 0

        lax.fori_loop(0, 5, one, 0)
        by_node[half, :, 640:TALL, :] = jnp.swapaxes(raw[half, 640:TALL], 0, 1)

    lane = lax.broadcasted_iota(jnp.int32, (LINES, 128), 1)
    action = lax.rem(lax.broadcasted_iota(jnp.int32, (LINES, 128), 0), ACT)

    def prepare(half, n, slot):
        if half == 1:
            pot_columns[slot] = turned(pot_rows[n])
        for block in range(6):
            lanes = pl.ds(block * 128, 128)
            flags = tall(live_rows[half, n, :, lanes], LINES)
            if block < 5:
                s_columns[slot, lanes, :] = turned(s_rows[half, n, :, lanes].astype(BF16))
                masked[slot, block] = by_node[half, n, lanes, :].T * flags
            else:
                column = turned(s_rows[half, n, :, lanes].astype(BF16))
                s_columns[slot, 640:TALL, :] = column[: TALL - 640]
                last = by_node[half, n, 640:TALL, :]
                last = jnp.concatenate([last, jnp.zeros((96, 128), BF16)], axis=0).T
                last = (last * flags).astype(F32)
                bar = jnp.where(action < counts[first + n], 0.0, -1024.0)
                bar = jnp.where(lane == HALF - 640, bar, 0.0)
                masked[slot, block] = jnp.where(lane < HALF - 640, last, bar).astype(BF16)

    def product(half, n, slot, tile):
        added = None
        for step, (start, height) in enumerate(K_TILES):
            inner = pl.ds(start, height)
            column = s_columns[slot, inner, :]
            signs = []
            for side in range(4):
                where = tile * 4 + side
                lanes = pl.ds((where % 6) * 128, 128)
                gap = tall(s_rows[where // 6, n, :, lanes], height) - column
                signs.append(
                    jnp.minimum(
                        jnp.maximum(gap, bounds[half, where, 1, inner, :]),
                        bounds[half, where, 0, inner, :],
                    )
                )
            left = jnp.concatenate([masked[slot, 2 * step], masked[slot, 2 * step + 1]], axis=1)
            term = jnp.dot(
                left[:, :height],
                jnp.concatenate(signs, axis=1),
                preferred_element_type=F32,
            )
            added = term if added is None else added + term
        return added

    def ahead(half, base, slots):
        for k, slot in enumerate(slots):
            last = base + k if isinstance(base, int) else jnp.minimum(base + k, MINE - 1)
            prepare(half, last, slot)

    def own_half(group, _):
        for part in range(2):
            ahead(0, 4 * group + 2 * part + 2, (2, 3) if part == 0 else (0, 1))
            for k in range(2):
                slot = 2 * part + k
                n = 4 * group + slot
                for tile in range(3):
                    partial[n, :, pl.ds(tile * 512, 512)] = product(0, n, slot, tile)
        return 0

    swap(0, lambda block: fetch(block).wait())
    ahead(0, 0, (0, 1))
    lax.fori_loop(0, EARLY, own_half, 0)
    pl.semaphore_wait(barrier, len(peers))
    for block in range(6):
        exchange(block).start()

    lane_row = lax.broadcasted_iota(jnp.int32, (1, 128), 1)
    spread = jnp.zeros((1, 128), jnp.int32)
    for n in range(LOCAL):
        spread = jnp.where(lane_row // 4 == n, parents[n], spread)
    key_row = (spread * 4 + lax.rem(lane_row, 4)).astype(F32)

    def key_copy(axis, step):
        return pltpu.make_async_remote_copy(
            src_ref=keys.at[axis, 0],
            dst_ref=keys.at[axis, sizes[axis] - step],
            send_sem=key_send.at[axis, step],
            recv_sem=key_recv.at[axis, sizes[axis] - step],
            device_id=at(along(axis, step), core),
            device_id_type=MESH_ID,
        )

    for axis in range(3):
        keys[axis, 0] = key_row
        for step in range(1, sizes[axis]):
            key_copy(axis, step).start()

    lax.fori_loop(EARLY, MINE // 4, own_half, 0)
    swap(1, lambda block: exchange(block).wait_recv())
    ahead(1, 0, (0, 1))

    my_block = core * (MINE * 4)

    def river_copies(group):
        copies = []
        from_rows = pl.ds(pl.multiple_of(group * 16, 16), 16)
        mine = pl.ds(pl.multiple_of(my_block + group * 16, 16), 16)
        for axis in range(3):
            send, recv = line_send.at[axis], line_recv.at[axis]
            for (step,) in far_first((sizes[axis],)):
                base = (sizes[axis] - step) * 128
                there = pl.ds(pl.multiple_of(base + my_block + group * 16, 16), 16)
                for source, which in (
                    (gathered.at[axis, mine], core),
                    (outgoing.at[axis, from_rows], far),
                ):
                    copies.append(
                        pltpu.make_async_remote_copy(
                            src_ref=source,
                            dst_ref=gathered.at[axis, there],
                            send_sem=send,
                            recv_sem=recv,
                            device_id=at(along(axis, step), which),
                            device_id_type=MESH_ID,
                        )
                    )
            copies.append(
                pltpu.make_async_remote_copy(
                    src_ref=outgoing.at[axis, from_rows],
                    dst_ref=gathered.at[axis, mine],
                    send_sem=send,
                    recv_sem=recv,
                    device_id=at(place, far),
                    device_id_type=MESH_ID,
                )
            )
        return copies

    def two_nodes(batch, part):
        ahead(1, 2 * batch + 2, (2, 3) if part == 0 else (0, 1))
        rivers = [[] for _ in range(6)]
        for tile in range(3):
            for slot in (2 * part, 2 * part + 1):
                n = 2 * batch + slot - 2 * part
                values = product(1, n, slot, tile) + partial[n, :, pl.ds(tile * 512, 512)]
                for pair in range(2):
                    chunk = tile * 2 + pair
                    for player in range(2):
                        for side in range(2):
                            start = (chunk % 3) * 256 + side * 128
                            parts = []
                            for g in range(GROUPS):
                                row = (player * GROUPS + g) * ACT
                                lane0 = pair * 256 + side * 128
                                piece = values[row : row + 8, lane0 : lane0 + 128]
                                parts.append(piece * pot_columns[slot, row : row + 8, :])
                            best = merged(parts, jnp.maximum)
                            flags = live_rows[chunk // 3, n, :, pl.ds(start, 128)]
                            rivers[chunk].append(best * flags)
        for chunk in range(6):
            block = merged(rivers[chunk], jnp.add)
            if chunk < 3:
                gathered[chunk, pl.ds(pl.multiple_of(my_block + batch * 8, 8), 8), :] = block
            else:
                outgoing[chunk - 3, pl.ds(pl.multiple_of(batch * 8, 8), 8), :] = block

    def four_nodes(group, _):
        two_nodes(2 * group, 0)
        two_nodes(2 * group + 1, 1)
        for copy in river_copies(group):
            copy.start()
        return 0

    lax.fori_loop(0, MINE // 4, four_nodes, 0)

    for axis in range(3):
        for step in range(1, sizes[axis]):
            key_copy(axis, step).wait_recv()

    for axis in range(3):
        count = plane_size(axis)
        q = lax.broadcasted_iota(jnp.int32, (count * 16, 128), 0)
        there = in_plane(axis, q // 16)
        owner = (there[0] * sizes[1] + there[1]) * sizes[2] + there[2]
        wanted = (owner * (TACT * 4) + lax.rem(q, 16)).astype(F32)
        for e in range(sizes[axis]):
            hit = jnp.where(wanted == keys[axis, e], 1.0, 0.0).astype(BF16)
            hot[axis, e, 0 : count * 16, :] = hit

    for axis in range(3):
        count = plane_size(axis)
        lines = sizes[axis] * 128
        blocks = (sizes[axis] - 1) * 128 + 64
        whole = gathered.at[axis, pl.ds(0, blocks)]
        pltpu.make_async_copy(whole, whole, line_recv.at[axis]).wait()
        rows_in = gathered[axis, pl.ds(0, lines), :]
        upper = rows_in.astype(BF16)
        lower = (rows_in - upper.astype(F32)).astype(BF16)
        left = jnp.concatenate(
            [hot[axis, e, 0 : count * 16, :] for e in range(sizes[axis])], axis=1
        )
        both = jnp.dot(
            left, jnp.concatenate([upper, lower], axis=1), preferred_element_type=F32
        )
        sums[axis, pl.ds(0, count * 16), :] = both[:, :128] + both[:, 128:]
        mine = plane_mine(axis)
        here = pl.ds(pl.multiple_of(mine * 16, 16), 16)
        high, low = planes[axis]
        for up, side in far_first((sizes[high], sizes[low])):
            where = list(place)
            where[high], where[low] = shifts[high][up], shifts[low][side]
            slot = where[high] * sizes[low] + where[low]
            part = pl.ds(pl.multiple_of(slot * 16, 16), 16)
            pltpu.make_async_remote_copy(
                src_ref=sums.at[axis, part],
                dst_ref=arrived.at[axis, here],
                send_sem=plane_send.at[axis],
                recv_sem=plane_recv.at[axis],
                device_id=at(where, core),
                device_id_type=MESH_ID,
            ).start()
        arrived[axis, here, :] = sums[axis, here, :]

    pltpu.make_async_copy(reach.at[turn], my_reach, reach_sem).wait()
    legal = turn_counts[turn]
    spot = lax.broadcasted_iota(jnp.int32, (1, 128), 1)
    weighed = jnp.zeros((1, 128), F32)
    for axis in range(3):
        count = plane_size(axis)
        whole = arrived.at[axis, pl.ds(0, (count - 1) * 16)]
        pltpu.make_async_copy(whole, whole, plane_recv.at[axis]).wait()
        total = arrived[axis, pl.ds(0, count * 16), :].reshape(count, 16, 128).sum(axis=0)
        best = total[0:4]
        for a in range(1, TACT):
            best = jnp.maximum(best, jnp.where(a < legal, total[4 * a : 4 * a + 4], -1e30))
        for player in range(2):
            for side in range(2):
                piece = best[player * 2 + side : player * 2 + side + 1]
                start = axis * 256 + side * 128
                width = min(128, HALF - start)
                lanes = pl.ds(start, width)
                turn_out[0, pl.ds(player, 1), lanes] = piece[:, :width]
                part = piece[:, :width] * my_reach[pl.ds(player, 1), lanes]
                if width == 128:
                    weighed = weighed + part
                else:
                    weighed = weighed + jnp.where(
                        spot == 0, jnp.sum(part, axis=1, keepdims=True), 0.0
                    )

    slot = turn * 2 + core
    my_part[0] = weighed
    parts_got[slot] = weighed
    for peer in peers:
        pltpu.make_async_remote_copy(
            src_ref=my_part.at[0],
            dst_ref=parts_got.at[slot],
            send_sem=part_send,
            recv_sem=part_recv,
            device_id=peer,
            device_id_type=MESH_ID,
        ).start()

    for block in range(6):
        exchange(block).wait_send()
    for axis in range(3):
        for step in range(1, sizes[axis]):
            key_copy(axis, step).wait_send()
        sent = gathered.at[axis, pl.ds(0, (sizes[axis] - 1) * 64)]
        for _ in range(2):
            pltpu.make_async_copy(sent, sent, line_send.at[axis]).wait()
        sent = gathered.at[axis, pl.ds(0, 64)]
        pltpu.make_async_copy(sent, sent, line_send.at[axis]).wait()
        sent = arrived.at[axis, pl.ds(0, (plane_size(axis) - 1) * 16)]
        pltpu.make_async_copy(sent, sent, plane_send.at[axis]).wait()
    sent = parts_got.at[pl.ds(0, len(peers))]
    pltpu.make_async_copy(sent, sent, part_send).wait()
    pltpu.make_async_copy(sent, sent, part_recv).wait()
    total_out[0, 0] = jnp.sum(parts_got[...].reshape(-1, 8, 1, 128).sum(axis=0).sum(axis=0))


def local(sizes, ranges, strengths, live, pots, counts, parents, turn_counts, reach):
    dma = pltpu.SemaphoreType.DMA
    longest = max(sizes)
    widest = max(sizes[0] * sizes[1], sizes[1] * sizes[2], sizes[0] * sizes[2])
    vmem = pl.BlockSpec(memory_space=pltpu.VMEM)
    smem = pl.BlockSpec(memory_space=pltpu.SMEM)
    hbm = pl.BlockSpec(memory_space=pl.ANY)
    turn_values, total = pl.pallas_call(
        functools.partial(kernel, sizes),
        out_shape=(
            jax.ShapeDtypeStruct((1, 2, HALF), F32),
            jax.ShapeDtypeStruct((1, 1), F32),
        ),
        in_specs=[hbm, hbm, hbm, hbm, smem, smem, smem, hbm, hbm],
        out_specs=(vmem, smem),
        scratch_shapes=[
            pltpu.VMEM((MINE, 2 * HALF), jnp.int32),
            pltpu.VMEM((MINE, 2 * HALF), jnp.int32),
            pltpu.VMEM((MINE, LINES), F32),
            pltpu.VMEM((4, WIDE, 64), BF16),
            pltpu.VMEM((2, TALL, MINE, LINES), BF16),
            pltpu.VMEM((2, MINE, TALL, LINES), BF16),
            pltpu.VMEM((4, 6, LINES, 128), BF16),
            pltpu.VMEM((2, MINE, 1, WIDE), F32),
            pltpu.VMEM((2, MINE, 1, WIDE), F32),
            pltpu.VMEM((MINE, 1, LINES), F32),
            pltpu.VMEM((4, TALL, 128), BF16),
            pltpu.VMEM((2, 12, 2, TALL + 16, 128), BF16),
            pltpu.VMEM((4, LINES, 128), F32),
            pltpu.VMEM((MINE, LINES, 2 * WIDE), F32),
            pltpu.VMEM((3, longest, widest * 16, 128), BF16),
            pltpu.VMEM((3, longest * 128, 128), F32),
            pltpu.VMEM((3, 64, 128), F32),
            pltpu.VMEM((3, longest, 1, 128), F32),
            pltpu.VMEM((3, widest * 16, 128), F32),
            pltpu.VMEM((3, widest * 16, 128), F32),
            pltpu.VMEM((2, HALF), F32),
            pltpu.VMEM((1, 1, 128), F32),
            pltpu.VMEM((sizes[0] * sizes[1] * sizes[2] * 2, 1, 128), F32),
            dma((6,)),
            dma((6,)),
            dma((6,)),
            dma((3,)),
            dma((3,)),
            dma((3, longest)),
            dma((3, longest)),
            dma((3,)),
            dma((3,)),
            dma(()),
            dma(()),
            dma(()),
            dma((4,)),
        ],
        compiler_params=pltpu.CompilerParams(
            collective_id=0,
            has_side_effects=True,
            vmem_limit_bytes=62 * 1024 * 1024,
        ),
    )(
        jnp.transpose(ranges, (2, 0, 1)),
        strengths,
        live,
        pots,
        counts,
        parents,
        turn_counts,
        reach,
        jnp.asarray(card_hots(), BF16),
    )
    return turn_values, total[0, 0]


def solution(mesh):
    sides = {128: (4, 4, 4), 16: (2, 2, 2)}[mesh.devices.size]
    split = Mesh(mesh.devices.reshape(*sides, 2), AXES)
    in_specs = (
        P(NODE, None, "hand"),
        P(NODE, None),
        P(NODE, None),
        P(NODE, None),
        P(NODE),
        P(NODE),
        P(),
        P(None, None, "hand"),
    )
    out_specs = (P(NODE, None, "hand"), P())
    return jax.shard_map(
        functools.partial(local, sides),
        mesh=split,
        in_specs=in_specs,
        out_specs=out_specs,
        check_vma=False,
    )
```

```python
import functools

import jax
import jax.numpy as jnp
import numpy as np
from jax import lax
from jax.experimental import pallas as pl
from jax.experimental.pallas import tpu as pltpu
from jax.sharding import Mesh
from jax.sharding import PartitionSpec as P

AXES = ("node_0", "node_1", "node_2", "hand")
NODE = AXES[:3]
MESH_ID = pl.DeviceIdType.MESH
F32 = jnp.float32
BF16 = jnp.bfloat16

ACT = 8
GROUPS = 8
TACT = 4
LINES = 128
HALF = 663
WIDE = 768
LOCAL = 32
MINE = 16
EARLY = 1
TALL = 672
K_TILES = ((0, 256), (256, 256), (512, 160))
J_BLOCKS = tuple((b * 128, min(128, HALF - b * 128)) for b in range(6))


def card_hots():
    first, second = np.triu_indices(52, 1)
    hots = np.zeros((4, WIDE, 64), np.float32)
    for half in range(2):
        for h in range(HALF):
            cards = [first[half * HALF + h], second[half * HALF + h]]
            hots[half, h, cards] = 1.0
            hots[2 + half, h, cards] = -1.0
            hots[2 + half, h, 52] = 1.0
        hots[half, :, 52] = 1.0
    return hots


def far_first(sides):
    steps = [step for step in np.ndindex(*sides) if any(step)]
    hops = [sum(min(at, side - at) for at, side in zip(step, sides)) for step in steps]
    return [steps[i] for i in np.argsort(-np.array(hops), kind="stable")]


def tall(row, rows):
    width = row.shape[1]
    block = jnp.broadcast_to(row, (16, width)).astype(BF16)
    return jnp.broadcast_to(block[None], (rows // 16, 16, width)).reshape(rows, width)


def turned(row):
    return jnp.broadcast_to(row, (128, 128)).T


def merged(parts, reduce):
    row = lax.broadcasted_iota(jnp.int32, (8, 128), 0)
    for bit in (1, 2, 4):
        low = (row & bit) == 0
        pairs = []
        for one, two in zip(parts[::2], parts[1::2]):
            kept = jnp.where(low, one, two)
            moved = pltpu.roll(jnp.where(low, two, one), 8 - bit, axis=0)
            pairs.append(reduce(kept, moved))
        parts = pairs
    return parts[0]


def kernel(
    sizes,
    ranges,
    strengths_in,
    live_in,
    pots_in,
    counts,
    parents,
    turn_counts,
    reach,
    hots_in,
    turn_out,
    total_out,
    strengths,
    live,
    pots,
    hots,
    raw,
    by_node,
    masked,
    s_rows,
    live_rows,
    pot_rows,
    s_columns,
    bounds,
    pot_columns,
    partial,
    hot,
    gathered,
    outgoing,
    keys,
    sums,
    arrived,
    my_reach,
    my_part,
    parts_got,
    own_sem,
    other_sem,
    ranges_send,
    line_recv,
    line_send,
    key_recv,
    key_send,
    plane_recv,
    plane_send,
    reach_sem,
    part_recv,
    part_send,
    small_sem,
):
    place = [lax.axis_index(name) for name in NODE]
    core = lax.axis_index("hand")
    far = 1 - core
    turn = (place[0] * sizes[1] + place[1]) * sizes[2] + place[2]
    planes = ((1, 2), (0, 2), (0, 1))

    def at(where, which):
        return (where[0], where[1], where[2], which)

    def along(axis, step):
        where = list(place)
        where[axis] = lax.rem(place[axis] + step, sizes[axis])
        return where

    def plane_size(axis):
        high, low = planes[axis]
        return sizes[high] * sizes[low]

    def plane_mine(axis):
        high, low = planes[axis]
        return place[high] * sizes[low] + place[low]

    def in_plane(axis, slot):
        high, low = planes[axis]
        where = list(place)
        where[high] = slot // sizes[low]
        where[low] = lax.rem(slot, sizes[low])
        return where

    shifts = [
        [lax.rem(place[axis] + step, sizes[axis]) for step in range(sizes[axis])]
        for axis in range(3)
    ]
    peers = [
        (shifts[0][i], shifts[1][j], shifts[2][k], (core, far)[other])
        for i, j, k, other in far_first((*sizes, 2))
    ]

    first = core * MINE
    def fetch(block):
        start, width = J_BLOCKS[block]
        return pltpu.make_async_copy(
            ranges.at[pl.ds(start, width), pl.ds(pl.multiple_of(first, MINE), MINE)],
            raw.at[0, pl.ds(start, width)],
            own_sem.at[block],
        )

    def exchange(block):
        start, width = J_BLOCKS[block]
        theirs = pl.ds(pl.multiple_of(far * MINE, MINE), MINE)
        return pltpu.make_async_remote_copy(
            src_ref=ranges.at[pl.ds(start, width), theirs],
            dst_ref=raw.at[1, pl.ds(start, width)],
            send_sem=ranges_send.at[block],
            recv_sem=other_sem.at[block],
            device_id=at(place, far),
            device_id_type=MESH_ID,
        )

    rows = pl.ds(pl.multiple_of(first, MINE), MINE)
    small = [
        pltpu.make_async_copy(source, target, small_sem.at[i])
        for i, (source, target) in enumerate(
            (
                (strengths_in.at[rows], strengths),
                (live_in.at[rows], live),
                (pots_in.at[rows], pots),
                (hots_in, hots),
            )
        )
    ]
    for copy in small:
        copy.start()
    for block in range(6):
        fetch(block).start()
    pltpu.make_async_copy(reach.at[turn], my_reach, reach_sem).start()

    barrier = pltpu.get_barrier_semaphore()
    for peer in peers:
        pl.semaphore_signal(barrier, inc=1, device_id=peer, device_id_type=MESH_ID)

    small[3].wait()

    def build(group, _):
        lanes = pl.ds(pl.multiple_of(group * 256, 256), 256)
        for j_half, j_core in enumerate((core, far)):
            for i_half, i_core in enumerate((core, far)):
                free = lax.dot_general(
                    hots[j_core, 0:TALL, :],
                    hots[2 + i_core, lanes, :],
                    (((1,), (1,)), ((), ())),
                    preferred_element_type=F32,
                ).astype(BF16)
                for side in range(2):
                    part = free[:, side * 128 : side * 128 + 128]
                    zero = jnp.zeros_like(part)
                    where = i_half * 6 + group * 2 + side
                    top = jnp.maximum(part, zero)
                    bounds[j_half, where, 0, 0:TALL, :] = top
                    bounds[j_half, where, 1, 0:TALL, :] = -top
        return 0

    lax.fori_loop(0, 3, build, 0)

    for copy in small[:3]:
        copy.wait()
    s_rows[...] = jnp.full_like(s_rows, -1000.0)
    live_rows[...] = jnp.zeros_like(live_rows)
    for source, target, shift in ((strengths, s_rows, 200.0), (live, live_rows, 0.0)):
        low = source[:, 0:HALF].astype(F32) - shift
        high = source[:, HALF : 2 * HALF].astype(F32) - shift
        mine, theirs = jnp.where(core == 0, low, high), jnp.where(core == 0, high, low)
        for n in range(MINE):
            target[0, n, :, 0:HALF] = mine[n : n + 1]
            target[1, n, :, 0:HALF] = theirs[n : n + 1]
    my_pots = pots[...]
    for n in range(MINE):
        pot_rows[n] = my_pots[n : n + 1]

    def swap(half, wait):
        for block in range(6):
            wait(block)

        def one(block, _):
            for part in range(4):
                rows = pl.ds(pl.multiple_of(block * 128 + part * 32, 32), 32)
                by_node[half, :, rows, :] = jnp.swapaxes(raw[half, rows], 0, 1)
            return 0

        lax.fori_loop(0, 5, one, 0)
        by_node[half, :, 640:TALL, :] = jnp.swapaxes(raw[half, 640:TALL], 0, 1)

    lane = lax.broadcasted_iota(jnp.int32, (LINES, 128), 1)
    action = lax.rem(lax.broadcasted_iota(jnp.int32, (LINES, 128), 0), ACT)

    def prepare(half, n, slot):
        if half == 1:
            pot_columns[slot] = turned(pot_rows[n])
        for block in range(6):
            lanes = pl.ds(block * 128, 128)
            flags = tall(live_rows[half, n, :, lanes], LINES)
            if block < 5:
                s_columns[slot, lanes, :] = turned(s_rows[half, n, :, lanes].astype(BF16))
                masked[slot, block] = by_node[half, n, lanes, :].T * flags
            else:
                column = turned(s_rows[half, n, :, lanes].astype(BF16))
                s_columns[slot, 640:TALL, :] = column[: TALL - 640]
                last = by_node[half, n, 640:TALL, :]
                last = jnp.concatenate([last, jnp.zeros((96, 128), BF16)], axis=0).T
                last = (last * flags).astype(F32)
                bar = jnp.where(action < counts[first + n], 0.0, -1024.0)
                bar = jnp.where(lane == HALF - 640, bar, 0.0)
                masked[slot, block] = jnp.where(lane < HALF - 640, last, bar).astype(BF16)

    def product(half, n, slot, tile):
        added = None
        for step, (start, height) in enumerate(K_TILES):
            inner = pl.ds(start, height)
            column = s_columns[slot, inner, :]
            signs = []
            for side in range(4):
                where = tile * 4 + side
                lanes = pl.ds((where % 6) * 128, 128)
                gap = tall(s_rows[where // 6, n, :, lanes], height) - column
                signs.append(
                    jnp.minimum(
                        jnp.maximum(gap, bounds[half, where, 1, inner, :]),
                        bounds[half, where, 0, inner, :],
                    )
                )
            left = jnp.concatenate([masked[slot, 2 * step], masked[slot, 2 * step + 1]], axis=1)
            term = jnp.dot(
                left[:, :height],
                jnp.concatenate(signs, axis=1),
                preferred_element_type=F32,
            )
            added = term if added is None else added + term
        return added

    def ahead(half, base, slots):
        for k, slot in enumerate(slots):
            last = base + k if isinstance(base, int) else jnp.minimum(base + k, MINE - 1)
            prepare(half, last, slot)

    def own_half(group, _):
        for part in range(2):
            ahead(0, 4 * group + 2 * part + 2, (2, 3) if part == 0 else (0, 1))
            for k in range(2):
                slot = 2 * part + k
                n = 4 * group + slot
                for tile in range(3):
                    partial[n, :, pl.ds(tile * 512, 512)] = product(0, n, slot, tile)
        return 0

    swap(0, lambda block: fetch(block).wait())
    ahead(0, 0, (0, 1))
    lax.fori_loop(0, EARLY, own_half, 0)
    pl.semaphore_wait(barrier, len(peers))
    for block in range(6):
        exchange(block).start()

    lane_row = lax.broadcasted_iota(jnp.int32, (1, 128), 1)
    spread = jnp.zeros((1, 128), jnp.int32)
    for n in range(LOCAL):
        spread = jnp.where(lane_row // 4 == n, parents[n], spread)
    key_row = (spread * 4 + lax.rem(lane_row, 4)).astype(F32)

    def key_copy(axis, step):
        return pltpu.make_async_remote_copy(
            src_ref=keys.at[axis, 0],
            dst_ref=keys.at[axis, sizes[axis] - step],
            send_sem=key_send.at[axis, step],
            recv_sem=key_recv.at[axis, sizes[axis] - step],
            device_id=at(along(axis, step), core),
            device_id_type=MESH_ID,
        )

    for axis in range(3):
        keys[axis, 0] = key_row
        for step in range(1, sizes[axis]):
            key_copy(axis, step).start()

    lax.fori_loop(EARLY, MINE // 4, own_half, 0)
    swap(1, lambda block: exchange(block).wait_recv())
    ahead(1, 0, (0, 1))

    my_block = core * (MINE * 4)

    def river_copies(group):
        copies = []
        from_rows = pl.ds(pl.multiple_of(group * 16, 16), 16)
        mine = pl.ds(pl.multiple_of(my_block + group * 16, 16), 16)
        for axis in range(3):
            send, recv = line_send.at[axis], line_recv.at[axis]
            for (step,) in far_first((sizes[axis],)):
                base = (sizes[axis] - step) * 128
                there = pl.ds(pl.multiple_of(base + my_block + group * 16, 16), 16)
                for source, which in (
                    (gathered.at[axis, mine], core),
                    (outgoing.at[axis, from_rows], far),
                ):
                    copies.append(
                        pltpu.make_async_remote_copy(
                            src_ref=source,
                            dst_ref=gathered.at[axis, there],
                            send_sem=send,
                            recv_sem=recv,
                            device_id=at(along(axis, step), which),
                            device_id_type=MESH_ID,
                        )
                    )
            copies.append(
                pltpu.make_async_remote_copy(
                    src_ref=outgoing.at[axis, from_rows],
                    dst_ref=gathered.at[axis, mine],
                    send_sem=send,
                    recv_sem=recv,
                    device_id=at(place, far),
                    device_id_type=MESH_ID,
                )
            )
        return copies

    def two_nodes(batch, part):
        ahead(1, 2 * batch + 2, (2, 3) if part == 0 else (0, 1))
        rivers = [[] for _ in range(6)]
        for tile in range(3):
            for slot in (2 * part, 2 * part + 1):
                n = 2 * batch + slot - 2 * part
                values = product(1, n, slot, tile) + partial[n, :, pl.ds(tile * 512, 512)]
                for pair in range(2):
                    chunk = tile * 2 + pair
                    for player in range(2):
                        for side in range(2):
                            start = (chunk % 3) * 256 + side * 128
                            parts = []
                            for g in range(GROUPS):
                                row = (player * GROUPS + g) * ACT
                                lane0 = pair * 256 + side * 128
                                piece = values[row : row + 8, lane0 : lane0 + 128]
                                parts.append(piece * pot_columns[slot, row : row + 8, :])
                            best = merged(parts, jnp.maximum)
                            flags = live_rows[chunk // 3, n, :, pl.ds(start, 128)]
                            rivers[chunk].append(best * flags)
        for chunk in range(6):
            block = merged(rivers[chunk], jnp.add)
            if chunk < 3:
                gathered[chunk, pl.ds(pl.multiple_of(my_block + batch * 8, 8), 8), :] = block
            else:
                outgoing[chunk - 3, pl.ds(pl.multiple_of(batch * 8, 8), 8), :] = block

    def four_nodes(group, _):
        two_nodes(2 * group, 0)
        two_nodes(2 * group + 1, 1)
        for copy in river_copies(group):
            copy.start()
        return 0

    lax.fori_loop(0, MINE // 4, four_nodes, 0)

    for axis in range(3):
        for step in range(1, sizes[axis]):
            key_copy(axis, step).wait_recv()

    for axis in range(3):
        count = plane_size(axis)
        q = lax.broadcasted_iota(jnp.int32, (count * 16, 128), 0)
        there = in_plane(axis, q // 16)
        owner = (there[0] * sizes[1] + there[1]) * sizes[2] + there[2]
        wanted = (owner * (TACT * 4) + lax.rem(q, 16)).astype(F32)
        for e in range(sizes[axis]):
            hit = jnp.where(wanted == keys[axis, e], 1.0, 0.0).astype(BF16)
            hot[axis, e, 0 : count * 16, :] = hit

    for axis in range(3):
        count = plane_size(axis)
        lines = sizes[axis] * 128
        blocks = (sizes[axis] - 1) * 128 + 64
        whole = gathered.at[axis, pl.ds(0, blocks)]
        pltpu.make_async_copy(whole, whole, line_recv.at[axis]).wait()
        rows_in = gathered[axis, pl.ds(0, lines), :]
        upper = rows_in.astype(BF16)
        lower = (rows_in - upper.astype(F32)).astype(BF16)
        left = jnp.concatenate(
            [hot[axis, e, 0 : count * 16, :] for e in range(sizes[axis])], axis=1
        )
        both = jnp.dot(
            left, jnp.concatenate([upper, lower], axis=1), preferred_element_type=F32
        )
        sums[axis, pl.ds(0, count * 16), :] = both[:, :128] + both[:, 128:]
        mine = plane_mine(axis)
        here = pl.ds(pl.multiple_of(mine * 16, 16), 16)
        high, low = planes[axis]
        for up, side in far_first((sizes[high], sizes[low])):
            where = list(place)
            where[high], where[low] = shifts[high][up], shifts[low][side]
            slot = where[high] * sizes[low] + where[low]
            part = pl.ds(pl.multiple_of(slot * 16, 16), 16)
            pltpu.make_async_remote_copy(
                src_ref=sums.at[axis, part],
                dst_ref=arrived.at[axis, here],
                send_sem=plane_send.at[axis],
                recv_sem=plane_recv.at[axis],
                device_id=at(where, core),
                device_id_type=MESH_ID,
            ).start()
        arrived[axis, here, :] = sums[axis, here, :]

    pltpu.make_async_copy(reach.at[turn], my_reach, reach_sem).wait()
    legal = turn_counts[turn]
    spot = lax.broadcasted_iota(jnp.int32, (1, 128), 1)
    weighed = jnp.zeros((1, 128), F32)
    for axis in range(3):
        count = plane_size(axis)
        whole = arrived.at[axis, pl.ds(0, (count - 1) * 16)]
        pltpu.make_async_copy(whole, whole, plane_recv.at[axis]).wait()
        total = arrived[axis, pl.ds(0, count * 16), :].reshape(count, 16, 128).sum(axis=0)
        best = total[0:4]
        for a in range(1, TACT):
            best = jnp.maximum(best, jnp.where(a < legal, total[4 * a : 4 * a + 4], -1e30))
        for player in range(2):
            for side in range(2):
                piece = best[player * 2 + side : player * 2 + side + 1]
                start = axis * 256 + side * 128
                width = min(128, HALF - start)
                lanes = pl.ds(start, width)
                turn_out[0, pl.ds(player, 1), lanes] = piece[:, :width]
                part = piece[:, :width] * my_reach[pl.ds(player, 1), lanes]
                if width == 128:
                    weighed = weighed + part
                else:
                    weighed = weighed + jnp.where(
                        spot == 0, jnp.sum(part, axis=1, keepdims=True), 0.0
                    )

    slot = turn * 2 + core
    my_part[0] = weighed
    parts_got[slot] = weighed
    for peer in peers:
        pltpu.make_async_remote_copy(
            src_ref=my_part.at[0],
            dst_ref=parts_got.at[slot],
            send_sem=part_send,
            recv_sem=part_recv,
            device_id=peer,
            device_id_type=MESH_ID,
        ).start()

    for block in range(6):
        exchange(block).wait_send()
    for axis in range(3):
        for step in range(1, sizes[axis]):
            key_copy(axis, step).wait_send()
        sent = gathered.at[axis, pl.ds(0, (sizes[axis] - 1) * 64)]
        for _ in range(2):
            pltpu.make_async_copy(sent, sent, line_send.at[axis]).wait()
        sent = gathered.at[axis, pl.ds(0, 64)]
        pltpu.make_async_copy(sent, sent, line_send.at[axis]).wait()
        sent = arrived.at[axis, pl.ds(0, (plane_size(axis) - 1) * 16)]
        pltpu.make_async_copy(sent, sent, plane_send.at[axis]).wait()
    sent = parts_got.at[pl.ds(0, len(peers))]
    pltpu.make_async_copy(sent, sent, part_send).wait()
    pltpu.make_async_copy(sent, sent, part_recv).wait()
    total_out[0, 0] = jnp.sum(parts_got[...].reshape(-1, 8, 1, 128).sum(axis=0).sum(axis=0))


def local(sizes, ranges, strengths, live, pots, counts, parents, turn_counts, reach):
    dma = pltpu.SemaphoreType.DMA
    longest = max(sizes)
    widest = max(sizes[0] * sizes[1], sizes[1] * sizes[2], sizes[0] * sizes[2])
    vmem = pl.BlockSpec(memory_space=pltpu.VMEM)
    smem = pl.BlockSpec(memory_space=pltpu.SMEM)
    hbm = pl.BlockSpec(memory_space=pl.ANY)
    turn_values, total = pl.pallas_call(
        functools.partial(kernel, sizes),
        out_shape=(
            jax.ShapeDtypeStruct((1, 2, HALF), F32),
            jax.ShapeDtypeStruct((1, 1), F32),
        ),
        in_specs=[hbm, hbm, hbm, hbm, smem, smem, smem, hbm, hbm],
        out_specs=(vmem, smem),
        scratch_shapes=[
            pltpu.VMEM((MINE, 2 * HALF), jnp.int32),
            pltpu.VMEM((MINE, 2 * HALF), jnp.int32),
            pltpu.VMEM((MINE, LINES), F32),
            pltpu.VMEM((4, WIDE, 64), BF16),
            pltpu.VMEM((2, TALL, MINE, LINES), BF16),
            pltpu.VMEM((2, MINE, TALL, LINES), BF16),
            pltpu.VMEM((4, 6, LINES, 128), BF16),
            pltpu.VMEM((2, MINE, 1, WIDE), F32),
            pltpu.VMEM((2, MINE, 1, WIDE), F32),
            pltpu.VMEM((MINE, 1, LINES), F32),
            pltpu.VMEM((4, TALL, 128), BF16),
            pltpu.VMEM((2, 12, 2, TALL + 16, 128), BF16),
            pltpu.VMEM((4, LINES, 128), F32),
            pltpu.VMEM((MINE, LINES, 2 * WIDE), F32),
            pltpu.VMEM((3, longest, widest * 16, 128), BF16),
            pltpu.VMEM((3, longest * 128, 128), F32),
            pltpu.VMEM((3, 64, 128), F32),
            pltpu.VMEM((3, longest, 1, 128), F32),
            pltpu.VMEM((3, widest * 16, 128), F32),
            pltpu.VMEM((3, widest * 16, 128), F32),
            pltpu.VMEM((2, HALF), F32),
            pltpu.VMEM((1, 1, 128), F32),
            pltpu.VMEM((sizes[0] * sizes[1] * sizes[2] * 2, 1, 128), F32),
            dma((6,)),
            dma((6,)),
            dma((6,)),
            dma((3,)),
            dma((3,)),
            dma((3, longest)),
            dma((3, longest)),
            dma((3,)),
            dma((3,)),
            dma(()),
            dma(()),
            dma(()),
            dma((4,)),
        ],
        compiler_params=pltpu.CompilerParams(
            collective_id=0,
            has_side_effects=True,
            vmem_limit_bytes=62 * 1024 * 1024,
        ),
    )(
        jnp.transpose(ranges, (2, 0, 1)),
        strengths,
        live,
        pots,
        counts,
        parents,
        turn_counts,
        reach,
        jnp.asarray(card_hots(), BF16),
    )
    return turn_values, total[0, 0]


def solution(mesh):
    sides = {128: (4, 4, 4), 16: (2, 2, 2)}[mesh.devices.size]
    split = Mesh(mesh.devices.reshape(*sides, 2), AXES)
    in_specs = (
        P(NODE, None, "hand"),
        P(NODE, None),
        P(NODE, None),
        P(NODE, None),
        P(NODE),
        P(NODE),
        P(),
        P(None, None, "hand"),
    )
    out_specs = (P(NODE, None, "hand"), P())
    return jax.shard_map(
        functools.partial(local, sides),
        mesh=split,
        in_specs=in_specs,
        out_specs=out_specs,
        check_vma=False,
    )
```
